256 devices in a mesh: row: 8 (over x, y_hi), col: 32 (over z, y_lo, core).
Axes of the slice: x: 4, y: 4 (y_hi: 2, y_lo: 2; y = y_hi * 2 + y_lo), z: 8, core: 2. Of those that a mesh axis runs over, the one named last changes fastest.
Arguments:
- boxes: int32 [4, 65536], P(None, 'col'), may hold values from 0 to 4095, as said below
- pins: int32 [65536], P('col'), may hold values from 2 to 64
- capacity: float32 [4096, 4096], P('row', 'col'), may hold values from 4 to 12
- cell_bin: int32 [8, 65536], P('row', 'col'), may hold values from 0 to 65535
- cell_area: float32 [8, 65536], P('row', 'col'), may hold values from 1 to 10
Outputs:
- rudy: float32 [4096, 4096], P('row', 'col')
- inflation: float32 [4096, 4096], P('row', 'col')
- cell_sizes: float32 [8, 65536], P('row', 'col')
The draws below stay inside these ranges and needn't reach their ends.
Inputs may be any that keep to these rules, and one draw needn't show every extreme that they name: `boxes`: row 0 and 1 are a net's first and last bin column, row 2 and 3 its first and last bin row; first <= last, a box spans at most 512 columns and 512 rows.
All inputs are finite; a program needn't handle non-finite values.
Results may differ from the reference program's by a relative error of at most 0.0003.
Values sent between devices are 32-bit elements; how exact they have to be, the bound alone decides.
No kernel may reach another device: no remote copies, remote signals or barrier semaphores. Data moves between devices by JAX's collectives and lax.ppermute only.
A program may use at most 64 MiB of HBM per device.

```python
import math
import jax
import jax.numpy as jnp

TILE_R = 512
TILE_C = 128
CELLS_DEV = 2048
GY = 4096
GX = 4096
NETS = 65536
SPAN_X = 512
SPAN_Y = 512
N_ROW = 8
N_COL = 32


def draw_boxes(key, part):
    keys = jax.random.split(key, 4)
    start_x = jax.random.randint(keys[0], (NETS,), 0, GX)
    width_x = jax.random.randint(keys[1], (NETS,), 1, SPAN_X + 1)
    start_y = jax.random.randint(keys[2], (NETS,), 0, GY)
    width_y = jax.random.randint(keys[3], (NETS,), 1, SPAN_Y + 1)
    end_x = jnp.minimum(start_x + width_x - 1, GX - 1)
    end_y = jnp.minimum(start_y + width_y - 1, GY - 1)
    return jnp.stack([start_x, end_x, start_y, end_y]).astype(jnp.int32)


def set_ends(values, stream_key, low, largest):
    index_at = [jax.random.randint(jax.random.fold_in(stream_key, axis), (), 0, length) for axis, length in enumerate(values.shape)]
    main_axis = values.shape.index(max(values.shape))
    next_to = index_at[:main_axis] + [(index_at[main_axis] + 1) % values.shape[main_axis]] + index_at[main_axis + 1:]
    return values.at[tuple(index_at)].set(low).at[tuple(next_to)].set(largest)


def steps_of(own_key, dims, shards, smallest, high):
    def one(axis_at, shards_of):
        draws = jax.random.uniform(jax.random.fold_in(jax.random.fold_in(own_key, 6), axis_at), (shards_of,), jnp.float32, smallest / len(shards), high / len(shards))
        return jnp.repeat(jnp.exp(draws), dims[axis_at] // shards_of).reshape((-1,) + (1,) * (len(dims) - axis_at - 1))

    loudness = one(*shards[0])
    for cut in shards[1:]:
        loudness = loudness * one(*cut)
    return loudness


def setup_inputs(seed: int = 0) -> dict:
    key_list = jax.random.split(jax.random.key(seed), 6)
    return {
        "boxes": draw_boxes(jax.random.fold_in(key_list[5], 71), 0),
        "pins": set_ends(jax.random.randint(key_list[1], (NETS,), 2, 65), jax.random.fold_in(key_list[1], 1), 2, 64).astype(jnp.int32),
        "capacity": jnp.clip(jnp.exp(math.log(12.0) - 1.0986123 * jax.random.uniform(key_list[2], (GY, GX), jnp.float32) ** steps_of(key_list[2], (GY, GX), ((0, 8), (1, 32)), -0.2, 0.2)), 4.0, 12.0),
        "cell_bin": set_ends(jax.random.randint(key_list[3], (N_ROW, N_COL * CELLS_DEV), 0, TILE_R * TILE_C), jax.random.fold_in(key_list[3], 1), 0, (TILE_R * TILE_C) - 1).astype(jnp.int32),
        "cell_area": jnp.clip(jnp.exp(math.log(10.0) - 2.3025851 * jax.random.uniform(key_list[4], (N_ROW, N_COL * CELLS_DEV), jnp.float32) ** steps_of(key_list[4], (N_ROW, N_COL * CELLS_DEV), ((0, 8), (1, 32)), -0.2, 0.2)), 1.0, 10.0),
    }


def net_weights(boxes, pins):
    span_x = (boxes[1] - boxes[0] + 1).astype(jnp.float32)
    span_y = (boxes[3] - boxes[2] + 1).astype(jnp.float32)
    weight = jnp.log(pins.astype(jnp.float32)) * (span_x + span_y) / (span_x * span_y)
    return weight.astype(jnp.bfloat16).astype(jnp.float32)


def reference(boxes, pins, capacity, cell_bin, cell_area):
    weight = net_weights(boxes, pins)
    first_x, last_x, first_y, last_y = boxes[0], boxes[1], boxes[2], boxes[3]
    corner = jnp.zeros((GY + 1, GX + 1), jnp.float32)
    corner = corner.at[first_y, first_x].add(weight)
    corner = corner.at[first_y, last_x + 1].add(-weight)
    corner = corner.at[last_y + 1, first_x].add(-weight)
    corner = corner.at[last_y + 1, last_x + 1].add(weight)
    rudy = jnp.cumsum(jnp.cumsum(corner, axis=0), axis=1)[:GY, :GX]
    excess = jnp.maximum(rudy - capacity, 0.0)
    prefix = jnp.cumsum(excess, axis=0)
    inflation = 1.0 + 2.0 * prefix / GY
    tile_row = jnp.arange(N_ROW, dtype=jnp.int32)[:, None]
    position = jnp.arange(N_COL * CELLS_DEV, dtype=jnp.int32)[None, :]
    bin_row = tile_row * TILE_R + cell_bin // TILE_C
    bin_col = (position // CELLS_DEV) * TILE_C + cell_bin % TILE_C
    grown = cell_area * inflation[bin_row, bin_col]
    cell_sizes = grown * (jnp.sum(cell_area) / jnp.sum(grown))
    return rudy, inflation, cell_sizes
```

```python
import functools

import jax
import jax.numpy as jnp
from jax import lax
from jax.experimental import pallas as pl
from jax.experimental.pallas import tpu as pltpu
from jax.sharding import Mesh
from jax.sharding import PartitionSpec as P

ROW = ("row_0", "row_1")
COL = ("col_0", "col_1", "col_2")
SLOTS = 128
LANES = 128
F32 = jnp.float32
BF16 = jnp.bfloat16


def iota(shape, dim):
    return lax.broadcasted_iota(jnp.int32, shape, dim)


def contract(a, b, dim_a, dim_b):
    return lax.dot_general(
        a, b, (((dim_a,), (dim_b,)), ((), ())), preferred_element_type=F32
    )


def three_parts(x):
    high = x.astype(BF16)
    rest = x - high.astype(F32)
    middle = rest.astype(BF16)
    low = (rest - middle.astype(F32)).astype(BF16)
    return high, middle, low


def pack_kernel(peers, groups, group_cols, tile_rows, info_ref, boxes_ref, pins_ref, out_ref, vals_ref):
    nets = boxes_ref.shape[1]
    row_start = info_ref[0]
    base = info_ref[1]
    first_x, last_x = boxes_ref[0:1, :], boxes_ref[1:2, :]
    first_y, last_y = boxes_ref[2:3, :], boxes_ref[3:4, :]
    span_x = (last_x - first_x + 1).astype(F32)
    span_y = (last_y - first_y + 1).astype(F32)
    weight = jnp.log(pins_ref[...].astype(F32)) * (span_x + span_y) / (span_x * span_y)
    weight = weight.astype(BF16).astype(F32)
    vals_ref[...] = jnp.zeros_like(vals_ref)
    vals_ref[0:4, :] = lax.shift_right_logical(boxes_ref[...], 8).astype(F32)
    vals_ref[4:5, :] = weight * (1.0 / 256.0)
    vals_ref[8:12, :] = (boxes_ref[...] & 255).astype(F32)
    vals = vals_ref[...].astype(BF16)

    group_at = iota((groups, nets), 0) * group_cols
    in_band = (first_y < row_start + tile_rows) & (last_y >= row_start)
    hit = (
        jnp.broadcast_to(in_band, (groups, nets))
        & (first_x < group_at + group_cols)
        & (last_x >= group_at)
    )
    hit = jnp.where(hit, 1.0, 0.0)
    chunks = nets // LANES
    stacked = jnp.concatenate(
        [hit[:, k * LANES : (k + 1) * LANES] for k in range(chunks)], axis=0
    ).astype(BF16)
    below = (iota((LANES, LANES), 0) < iota((LANES, LANES), 1)).astype(F32).astype(BF16)
    before = contract(stacked, below, 1, 0)
    whole = contract(stacked, jnp.ones((LANES, LANES), BF16), 1, 0)
    offset = jnp.zeros((groups, LANES), F32)
    ranks = []
    for k in range(chunks):
        rows = slice(k * groups, (k + 1) * groups)
        ranks.append(before[rows] + offset)
        offset = offset + whole[rows]
    rank = jnp.concatenate(ranks, axis=1)
    rank = jnp.where(hit > 0.0, rank - base.astype(F32), -1.0)
    largest = jnp.max(offset, axis=0, keepdims=True)

    slot = iota((SLOTS, nets), 0).astype(F32)
    field = iota((8, SLOTS), 0)
    for group in range(groups):
        chosen = jnp.where(slot == rank[group : group + 1, :], 1.0, 0.0).astype(BF16)
        got = contract(vals, chosen, 1, 1)
        row = got[0:8] * 256.0 + got[8:16]
        row = jnp.where(field == 5, jnp.broadcast_to(largest, (8, SLOTS)), row)
        for peer in range(group * (peers // groups), (group + 1) * (peers // groups)):
            out_ref[peer] = row


def tile_kernel(
    row_peers,
    info_ref,
    nets_ref,
    past_ref,
    capacity_ref,
    bins_ref,
    area_ref,
    rudy_ref,
    within_ref,
    looked_ref,
    pay_ref,
    hits_ref,
    cols_ref,
):
    tile_rows, tile_cols = capacity_ref.shape
    row_start = info_ref[0]
    col_start = info_ref[1]
    first_round = info_ref[2]
    peers = nets_ref.shape[0]
    row_at = (iota((tile_rows, SLOTS), 0) + row_start).astype(F32)
    col_at = (iota((tile_cols, SLOTS), 0) + col_start).astype(F32)
    largest = jnp.zeros((1, SLOTS), F32)
    for peer in range(peers):
        box = nets_ref[peer]
        first_x, last_x = box[0:1], box[1:2]
        first_y, last_y = box[2:3], box[3:4]
        weight = box[4:5]
        largest = jnp.maximum(largest, box[5:6])
        at = slice(peer * SLOTS, (peer + 1) * SLOTS)
        hits_ref[:, at] = jnp.where(
            (row_at >= first_y) & (row_at <= last_y), 1.0, 0.0
        ).astype(BF16)
        cols_ref[:, at] = jnp.where(
            (col_at >= first_x) & (col_at <= last_x),
            jnp.broadcast_to(weight, col_at.shape),
            0.0,
        ).astype(BF16)
    rudy = contract(hits_ref[...], cols_ref[...], 1, 1)
    rudy = rudy + jnp.where(first_round == 0, 0.0, past_ref[...])
    rudy_ref[...] = rudy
    excess = jnp.maximum(rudy - capacity_ref[...], 0.0)

    half = 256
    lower = (iota((half, half), 0) >= iota((half, half), 1)).astype(F32).astype(BF16)
    carry = jnp.zeros((1, tile_cols), F32)
    parts = []
    for start in range(0, tile_rows, half):
        pieces = jnp.concatenate(three_parts(excess[start : start + half]), axis=1)
        sums = contract(lower, pieces, 1, 0)
        part = (
            sums[:, :tile_cols]
            + sums[:, tile_cols : 2 * tile_cols]
            + sums[:, 2 * tile_cols :]
            + carry
        )
        parts.append(part)
        carry = part[half - 1 : half, :]
    within = jnp.concatenate(parts, axis=0)
    within_ref[...] = within

    cells = bins_ref.shape[1]
    bin_row = lax.shift_right_logical(bins_ref[...], 7)
    bin_col = bins_ref[...] & 127
    area = area_ref[...]
    row_hot = jnp.where(iota((tile_rows, cells), 0) == bin_row, 1.0, 0.0).astype(BF16)
    is_col = iota((tile_cols, cells), 0) == bin_col
    turned = jnp.concatenate(three_parts(within.T), axis=0)
    picked = contract(turned, row_hot, 1, 0)
    picked = (
        picked[:tile_cols] + picked[tile_cols : 2 * tile_cols] + picked[2 * tile_cols :]
    )
    looked = jnp.sum(jnp.where(is_col, picked, 0.0), axis=0, keepdims=True)
    looked_ref[...] = looked

    high, middle, low = three_parts(area)
    pieces = jnp.concatenate(
        [high.astype(F32), middle.astype(F32), low.astype(F32), jnp.zeros((5, cells), F32)],
        axis=0,
    ).astype(BF16)
    col_area = contract(pieces, jnp.where(is_col, 1.0, 0.0).astype(BF16), 1, 1)
    col_area = jnp.sum(col_area, axis=0, keepdims=True)
    weighed = area * looked
    area_sum = area[:, :LANES]
    weighed_sum = weighed[:, :LANES]
    for k in range(1, cells // LANES):
        area_sum = area_sum + area[:, k * LANES : (k + 1) * LANES]
        weighed_sum = weighed_sum + weighed[:, k * LANES : (k + 1) * LANES]
    field = iota((8, LANES), 0)
    pay = jnp.zeros((8, LANES), F32)
    for at, row in enumerate((carry, col_area, area_sum, weighed_sum, largest)):
        pay = jnp.where(field == at, jnp.broadcast_to(row, (8, LANES)), pay)
    for peer in range(row_peers):
        pay_ref[peer] = pay


def carry_kernel(col_peers, factor, info_ref, pays_ref, carried_ref, totals_ref):
    me = info_ref[0]
    running = jnp.zeros((1, LANES), F32)
    mine = jnp.zeros((1, LANES), F32)
    area_sum = jnp.zeros((1, LANES), F32)
    weighed = jnp.zeros((1, LANES), F32)
    for peer in range(pays_ref.shape[0]):
        pay = pays_ref[peer]
        mine = jnp.where(me == peer, running, mine)
        area_sum = area_sum + pay[2:3]
        weighed = weighed + pay[3:4] + pay[1:2] * running
        running = running + pay[0:1]
    carried_ref[...] = jnp.broadcast_to(mine, carried_ref.shape)
    field = iota((8, LANES), 0)
    totals = jnp.where(
        field == 0,
        jnp.broadcast_to(area_sum, (8, LANES)),
        jnp.broadcast_to(area_sum + factor * weighed, (8, LANES)),
    )
    for peer in range(col_peers):
        totals_ref[peer] = totals


def final_kernel(
    factor,
    within_ref,
    carried_ref,
    totals_ref,
    bins_ref,
    area_ref,
    looked_ref,
    inflation_ref,
    sizes_ref,
):
    carried = carried_ref[...]
    inflation_ref[...] = 1.0 + factor * (within_ref[...] + carried[0:1])
    totals = jnp.sum(totals_ref[...], axis=0)
    area_total = jnp.sum(totals[0:1], axis=1, keepdims=True)
    grown_total = jnp.sum(totals[1:2], axis=1, keepdims=True)
    bin_col = bins_ref[...] & 127
    rows = bin_col.shape[0]
    above = jnp.take_along_axis(
        jnp.broadcast_to(carried[0:1], (rows, LANES)), bin_col, axis=1
    )
    grown = area_ref[...] * (1.0 + factor * (looked_ref[...] + above))
    sizes_ref[...] = grown * (area_total / grown_total)


def call(kernel, out_shapes, args, scratch=(), flops=1_000_000):
    smem = pl.BlockSpec(memory_space=pltpu.SMEM)
    vmem = pl.BlockSpec(memory_space=pltpu.VMEM)
    specs = [smem if a.ndim == 1 else vmem for a in args]
    return pl.pallas_call(
        kernel,
        out_shape=[jax.ShapeDtypeStruct(s, F32) for s in out_shapes],
        in_specs=specs,
        out_specs=[vmem for _ in out_shapes],
        scratch_shapes=list(scratch),
        cost_estimate=pl.CostEstimate(flops=flops, bytes_accessed=1_000_000, transcendentals=0),
    )(*args)


def exchange(payload, axis):
    return lax.all_to_all(payload, axis, 0, 0, tiled=True)


def per_device(boxes, pins, capacity, cell_bin, cell_area):
    tile_rows, tile_cols = capacity.shape
    rows, cols = lax.axis_size(ROW), lax.axis_size(COL)
    groups = lax.axis_size("col_0")
    nets = boxes.shape[1]
    cells = cell_bin.shape[1]
    factor = 2.0 / (tile_rows * rows)
    row_at = lax.axis_index(ROW)
    row_start = row_at * tile_rows
    col_start = lax.axis_index(COL) * tile_cols
    pins = pins.reshape(1, nets)

    def one_round(index, past):
        base = index * SLOTS
        (packed,) = call(
            functools.partial(
                pack_kernel, cols, groups, tile_cols * (cols // groups), tile_rows
            ),
            [(cols, 8, SLOTS)],
            (jnp.stack([row_start, base]), boxes, pins),
            [pltpu.VMEM((16, nets), F32)],
            10_000_000_000,
        )
        mine = exchange(packed, COL)
        rudy, within, looked, pay = call(
            functools.partial(tile_kernel, rows),
            [(tile_rows, tile_cols), (tile_rows, tile_cols), (1, cells), (rows, 8, LANES)],
            (jnp.stack([row_start, col_start, index]), mine, past, capacity, cell_bin, cell_area),
            [
                pltpu.VMEM((tile_rows, cols * SLOTS), BF16),
                pltpu.VMEM((tile_cols, cols * SLOTS), BF16),
            ],
            10_000_000_000,
        )
        return rudy, within, looked, exchange(pay, ROW)

    def unfinished(state):
        index, _, _, _, pays = state
        return jnp.max(pays[:, 4, 0]) > (index * SLOTS).astype(F32)

    def next_round(state):
        index, rudy, _, _, _ = state
        return (index + 1, *one_round(index, rudy))

    first = (jnp.int32(1), *one_round(jnp.int32(0), capacity))
    _, rudy, within, looked, pays = lax.while_loop(unfinished, next_round, first)

    carried, totals = call(
        functools.partial(carry_kernel, cols, factor),
        [(8, LANES), (cols, 8, LANES)],
        (row_at[None], pays),
    )
    totals = exchange(totals, COL)
    shape = (cells // LANES, LANES)
    inflation, sizes = call(
        functools.partial(final_kernel, factor),
        [(tile_rows, tile_cols), shape],
        (
            within,
            carried,
            totals,
            cell_bin.reshape(shape),
            cell_area.reshape(shape),
            looked.reshape(shape),
        ),
    )
    return rudy, inflation, sizes.reshape(cell_area.shape)


def solution(mesh):
    split = Mesh(mesh.devices.reshape(4, 2, 8, 2, 2), ROW + COL)
    placed = (P(None, COL), P(COL), P(ROW, COL), P(ROW, COL), P(ROW, COL))
    return jax.shard_map(
        per_device,
        mesh=split,
        in_specs=placed,
        out_specs=(P(ROW, COL), P(ROW, COL), P(ROW, COL)),
        check_vma=False,
    )
```

```python
import functools

import jax
import jax.numpy as jnp
from jax import lax
from jax.experimental import pallas as pl
from jax.experimental.pallas import tpu as pltpu
from jax.sharding import Mesh
from jax.sharding import PartitionSpec as P

ROW = ("row_0", "row_1")
COL = ("col_0", "col_1", "col_2")
SLOTS = 128
LANES = 128
F32 = jnp.float32
BF16 = jnp.bfloat16


def iota(shape, dim):
    return lax.broadcasted_iota(jnp.int32, shape, dim)


def contract(a, b, dim_a, dim_b):
    return lax.dot_general(
        a, b, (((dim_a,), (dim_b,)), ((), ())), preferred_element_type=F32
    )


def three_parts(x):
    high = x.astype(BF16)
    rest = x - high.astype(F32)
    middle = rest.astype(BF16)
    low = (rest - middle.astype(F32)).astype(BF16)
    return high, middle, low


def pack_kernel(
    peers, groups, group_cols, tile_rows, row_ref, base_ref, boxes_ref, pins_ref, out_ref, vals_ref
):
    nets = boxes_ref.shape[1]
    row_start = row_ref[0]
    base = base_ref[0]
    first_x, last_x = boxes_ref[0:1, :], boxes_ref[1:2, :]
    first_y, last_y = boxes_ref[2:3, :], boxes_ref[3:4, :]
    span_x = (last_x - first_x + 1).astype(F32)
    span_y = (last_y - first_y + 1).astype(F32)
    weight = jnp.log(pins_ref[...].astype(F32)) * (span_x + span_y) / (span_x * span_y)
    weight = weight.astype(BF16).astype(F32)
    vals_ref[...] = jnp.zeros_like(vals_ref)
    vals_ref[0:4, :] = lax.shift_right_logical(boxes_ref[...], 8).astype(F32)
    vals_ref[4:5, :] = weight * (1.0 / 256.0)
    vals_ref[8:12, :] = (boxes_ref[...] & 255).astype(F32)
    vals = vals_ref[...].astype(BF16)

    group_at = iota((groups, nets), 0) * group_cols
    in_band = (first_y < row_start + tile_rows) & (last_y >= row_start)
    hit = (
        jnp.broadcast_to(in_band, (groups, nets))
        & (first_x < group_at + group_cols)
        & (last_x >= group_at)
    )
    hit = jnp.where(hit, 1.0, 0.0)
    chunks = nets // LANES
    stacked = jnp.concatenate(
        [hit[:, k * LANES : (k + 1) * LANES] for k in range(chunks)], axis=0
    ).astype(BF16)
    below = (iota((LANES, LANES), 0) < iota((LANES, LANES), 1)).astype(F32).astype(BF16)
    before = contract(stacked, below, 1, 0)
    whole = contract(stacked, jnp.ones((LANES, LANES), BF16), 1, 0)
    offset = jnp.zeros((groups, LANES), F32)
    ranks = []
    for k in range(chunks):
        rows = slice(k * groups, (k + 1) * groups)
        ranks.append(before[rows] + offset)
        offset = offset + whole[rows]
    rank = jnp.concatenate(ranks, axis=1)
    rank = jnp.where(hit > 0.0, rank - base.astype(F32), -1.0)
    largest = jnp.max(offset, axis=0, keepdims=True)

    slot = iota((SLOTS, nets), 0).astype(F32)
    field = iota((8, SLOTS), 0)
    for group in range(groups):
        chosen = jnp.where(slot == rank[group : group + 1, :], 1.0, 0.0).astype(BF16)
        got = contract(vals, chosen, 1, 1)
        row = got[0:8] * 256.0 + got[8:16]
        row = jnp.where(field == 5, jnp.broadcast_to(largest, (8, SLOTS)), row)
        for peer in range(group * (peers // groups), (group + 1) * (peers // groups)):
            out_ref[peer] = row


def cells_kernel(tile_rows, tile_cols, bins_ref, area_ref, row_hot_ref, col_hot_ref, sums_ref):
    cells = bins_ref.shape[1]
    bin_row = lax.shift_right_logical(bins_ref[...], 7)
    bin_col = bins_ref[...] & 127
    area = area_ref[...]
    row_hot_ref[...] = jnp.where(iota((tile_rows, cells), 0) == bin_row, 1.0, 0.0).astype(BF16)
    col_hot = jnp.where(iota((tile_cols, cells), 0) == bin_col, 1.0, 0.0).astype(BF16)
    col_hot_ref[...] = col_hot
    high, middle, low = three_parts(area)
    pieces = jnp.concatenate(
        [high.astype(F32), middle.astype(F32), low.astype(F32), jnp.zeros((5, cells), F32)],
        axis=0,
    ).astype(BF16)
    col_area = jnp.sum(contract(pieces, col_hot, 1, 1), axis=0, keepdims=True)
    area_sum = lane_sums(area)
    at = iota((8, LANES), 0)
    sums_ref[...] = jnp.where(
        at == 0,
        jnp.broadcast_to(col_area, (8, LANES)),
        jnp.broadcast_to(area_sum, (8, LANES)),
    )


def lane_sums(row):
    total = row[:, :LANES]
    for k in range(1, row.shape[1] // LANES):
        total = total + row[:, k * LANES : (k + 1) * LANES]
    return total


def tile_kernel(
    row_peers,
    has_past,
    row_ref,
    col_ref,
    nets_ref,
    capacity_ref,
    area_ref,
    row_hot_ref,
    col_hot_ref,
    sums_ref,
    *refs,
):
    if has_past:
        past_ref, *refs = refs
    rudy_ref, within_ref, looked_ref, pay_ref, hits_ref, cols_ref = refs
    tile_rows, tile_cols = capacity_ref.shape
    row_start = row_ref[0]
    col_start = col_ref[0]
    peers = nets_ref.shape[0]
    row_at = (iota((tile_rows, SLOTS), 0) + row_start).astype(F32)
    col_at = (iota((tile_cols, SLOTS), 0) + col_start).astype(F32)
    largest = jnp.zeros((1, SLOTS), F32)
    for peer in range(peers):
        box = nets_ref[peer]
        first_x, last_x = box[0:1], box[1:2]
        first_y, last_y = box[2:3], box[3:4]
        weight = box[4:5]
        largest = jnp.maximum(largest, box[5:6])
        at = slice(peer * SLOTS, (peer + 1) * SLOTS)
        hits_ref[:, at] = jnp.where(
            (row_at >= first_y) & (row_at <= last_y), 1.0, 0.0
        ).astype(BF16)
        cols_ref[:, at] = jnp.where(
            (col_at >= first_x) & (col_at <= last_x),
            jnp.broadcast_to(weight, col_at.shape),
            0.0,
        ).astype(BF16)
    rudy = contract(hits_ref[...], cols_ref[...], 1, 1)
    if has_past:
        rudy = rudy + past_ref[...]
    rudy_ref[...] = rudy
    excess = jnp.maximum(rudy - capacity_ref[...], 0.0)

    half = 256
    lower = (iota((half, half), 0) >= iota((half, half), 1)).astype(F32).astype(BF16)
    carry = jnp.zeros((1, tile_cols), F32)
    parts = []
    for start in range(0, tile_rows, half):
        pieces = jnp.concatenate(three_parts(excess[start : start + half]), axis=1)
        sums = contract(lower, pieces, 1, 0)
        part = (
            sums[:, :tile_cols]
            + sums[:, tile_cols : 2 * tile_cols]
            + sums[:, 2 * tile_cols :]
            + carry
        )
        parts.append(part)
        carry = part[half - 1 : half, :]
    within = jnp.concatenate(parts, axis=0)
    within_ref[...] = within

    turned = jnp.concatenate(three_parts(within.T), axis=0)
    picked = contract(turned, row_hot_ref[...], 1, 0)
    picked = (
        picked[:tile_cols] + picked[tile_cols : 2 * tile_cols] + picked[2 * tile_cols :]
    )
    looked = jnp.sum(picked * col_hot_ref[...].astype(F32), axis=0, keepdims=True)
    looked_ref[...] = looked
    weighed_sum = lane_sums(area_ref[...] * looked)
    at = iota((8, LANES), 0)
    pay = jnp.zeros((8, LANES), F32)
    for k, row in enumerate((carry, sums_ref[0:1], sums_ref[1:2], weighed_sum, largest)):
        pay = jnp.where(at == k, jnp.broadcast_to(row, (8, LANES)), pay)
    for peer in range(row_peers):
        pay_ref[peer] = pay


def carry_kernel(col_peers, factor, me_ref, pays_ref, carried_ref, totals_ref, most_ref):
    me = me_ref[0]
    running = jnp.zeros((1, LANES), F32)
    mine = jnp.zeros((1, LANES), F32)
    area_sum = jnp.zeros((1, LANES), F32)
    weighed = jnp.zeros((1, LANES), F32)
    largest = jnp.zeros((1, LANES), F32)
    for peer in range(pays_ref.shape[0]):
        pay = pays_ref[peer]
        mine = jnp.where(me == peer, running, mine)
        area_sum = area_sum + pay[2:3]
        weighed = weighed + pay[3:4] + pay[1:2] * running
        largest = jnp.maximum(largest, pay[4:5])
        running = running + pay[0:1]
    most_ref[0] = jnp.max(largest)
    carried_ref[...] = jnp.broadcast_to(mine, carried_ref.shape)
    grown = area_sum + factor * weighed
    half = LANES // 2
    both = jnp.where(
        iota((1, LANES), 1) < half,
        area_sum + pltpu.roll(area_sum, half, 1),
        grown + pltpu.roll(grown, half, 1),
    )
    totals_ref[...] = jnp.broadcast_to(both, totals_ref.shape)


def final_kernel(
    factor,
    within_ref,
    carried_ref,
    totals_ref,
    bins_ref,
    area_ref,
    looked_ref,
    inflation_ref,
    sizes_ref,
):
    carried = carried_ref[...]
    inflation_ref[...] = 1.0 + factor * (within_ref[...] + carried[0:1])
    totals = jnp.sum(totals_ref[...], axis=0, keepdims=True)
    lower = iota(totals.shape, 1) < LANES // 2
    area_total = jnp.sum(jnp.where(lower, totals, 0.0), axis=1, keepdims=True)
    grown_total = jnp.sum(jnp.where(lower, 0.0, totals), axis=1, keepdims=True)
    bin_col = bins_ref[...] & 127
    rows = bin_col.shape[0]
    above = jnp.take_along_axis(
        jnp.broadcast_to(carried[0:1], (rows, LANES)), bin_col, axis=1
    )
    grown = area_ref[...] * (1.0 + factor * (looked_ref[...] + above))
    sizes_ref[...] = grown * (area_total / grown_total)


def call(kernel, outs, args, scratch=(), limit=16, flops=1_000_000):
    smem = pl.BlockSpec(memory_space=pltpu.SMEM)
    vmem = pl.BlockSpec(memory_space=pltpu.VMEM)
    outs = [o if isinstance(o, jax.ShapeDtypeStruct) else jax.ShapeDtypeStruct(o, F32) for o in outs]
    return pl.pallas_call(
        kernel,
        out_shape=outs,
        in_specs=[smem if a.ndim == 1 else vmem for a in args],
        out_specs=[smem if len(o.shape) == 1 else vmem for o in outs],
        scratch_shapes=list(scratch),
        compiler_params=pltpu.CompilerParams(vmem_limit_bytes=limit * 1024 * 1024),
        cost_estimate=pl.CostEstimate(flops=flops, bytes_accessed=1_000_000, transcendentals=0),
    )(*args)


def exchange(payload, axis):
    return lax.all_to_all(payload, axis, 0, 0, tiled=True)


def per_device(boxes, pins, capacity, cell_bin, cell_area):
    tile_rows, tile_cols = capacity.shape
    rows, cols = lax.axis_size(ROW), lax.axis_size(COL)
    groups = lax.axis_size("col_0")
    nets = boxes.shape[1]
    cells = cell_bin.shape[1]
    factor = 2.0 / (tile_rows * rows)
    row_at = lax.axis_index(ROW)[None]
    row_start = row_at * tile_rows
    col_start = lax.axis_index(COL)[None] * tile_cols
    pins = pins.reshape(1, nets)
    row_hot, col_hot, cell_sums = call(
        functools.partial(cells_kernel, tile_rows, tile_cols),
        [
            jax.ShapeDtypeStruct((tile_rows, cells), BF16),
            jax.ShapeDtypeStruct((tile_cols, cells), BF16),
            (8, LANES),
        ],
        (cell_bin, cell_area),
        flops=4_000_000_000,
    )

    def one_round(index, past):
        (packed,) = call(
            functools.partial(
                pack_kernel, cols, groups, tile_cols * (cols // groups), tile_rows
            ),
            [(cols, 8, SLOTS)],
            (row_start, index[None] * SLOTS, boxes, pins),
            [pltpu.VMEM((16, nets), F32)],
        )
        mine = exchange(packed, COL)
        rudy, within, looked, pay = call(
            functools.partial(tile_kernel, rows, past is not None),
            [(tile_rows, tile_cols), (tile_rows, tile_cols), (1, cells), (rows, 8, LANES)],
            (row_start, col_start, mine, capacity, cell_area, row_hot, col_hot, cell_sums)
            + (() if past is None else (past,)),
            [
                pltpu.VMEM((tile_rows, cols * SLOTS), BF16),
                pltpu.VMEM((tile_cols, cols * SLOTS), BF16),
            ],
            limit=28,
        )
        carried, totals, most = call(
            functools.partial(carry_kernel, cols, factor),
            [(8, LANES), (cols, LANES), (1,)],
            (row_at, exchange(pay, ROW)),
        )
        return index + 1, most, rudy, within, looked, carried, totals

    def unfinished(state):
        index, most, *_ = state
        return most[0] > (index * SLOTS).astype(F32)

    def next_round(state):
        return one_round(state[0], state[2])

    first = one_round(jnp.int32(0), None)
    _, _, rudy, within, looked, carried, totals = lax.while_loop(unfinished, next_round, first)

    totals = exchange(totals, COL)
    shape = (cells // LANES, LANES)
    inflation, sizes = call(
        functools.partial(final_kernel, factor),
        [(tile_rows, tile_cols), shape],
        (
            within,
            carried,
            totals,
            cell_bin.reshape(shape),
            cell_area.reshape(shape),
            looked.reshape(shape),
        ),
    )
    return rudy, inflation, sizes.reshape(cell_area.shape)


def solution(mesh):
    split = Mesh(mesh.devices.reshape(4, 2, 8, 2, 2), ROW + COL)
    placed = (P(None, COL), P(COL), P(ROW, COL), P(ROW, COL), P(ROW, COL))
    return jax.shard_map(
        per_device,
        mesh=split,
        in_specs=placed,
        out_specs=(P(ROW, COL), P(ROW, COL), P(ROW, COL)),
        check_vma=False,
    )
```

```python
import functools

import jax
import jax.numpy as jnp
from jax import lax
from jax.experimental import pallas as pl
from jax.experimental.pallas import tpu as pltpu
from jax.sharding import Mesh
from jax.sharding import PartitionSpec as P

ROW = ("row_0", "row_1")
COL = ("col_0", "col_1", "col_2")
SLOTS = 128
LANES = 128
F32 = jnp.float32
BF16 = jnp.bfloat16


def iota(shape, dim):
    return lax.broadcasted_iota(jnp.int32, shape, dim)


def contract(a, b, dim_a, dim_b):
    return lax.dot_general(
        a, b, (((dim_a,), (dim_b,)), ((), ())), preferred_element_type=F32
    )


def three_parts(x):
    high = x.astype(BF16)
    rest = x - high.astype(F32)
    middle = rest.astype(BF16)
    low = (rest - middle.astype(F32)).astype(BF16)
    return high, middle, low


def pack_kernel(
    peers, groups, group_cols, tile_rows, row_ref, base_ref, boxes_ref, pins_ref, out_ref, vals_ref
):
    nets = boxes_ref.shape[1]
    row_start = row_ref[0]
    base = base_ref[0]
    first_x, last_x = boxes_ref[0:1, :], boxes_ref[1:2, :]
    first_y, last_y = boxes_ref[2:3, :], boxes_ref[3:4, :]
    span_x = (last_x - first_x + 1).astype(F32)
    span_y = (last_y - first_y + 1).astype(F32)
    weight = jnp.log(pins_ref[...].astype(F32)) * (span_x + span_y) / (span_x * span_y)
    weight = weight.astype(BF16).astype(F32)
    vals_ref[...] = jnp.zeros_like(vals_ref)
    vals_ref[0:4, :] = lax.shift_right_logical(boxes_ref[...], 8).astype(F32)
    vals_ref[4:5, :] = weight * (1.0 / 256.0)
    vals_ref[8:12, :] = (boxes_ref[...] & 255).astype(F32)
    vals = vals_ref[...].astype(BF16)

    group_at = iota((groups, nets), 0) * group_cols
    in_band = (first_y < row_start + tile_rows) & (last_y >= row_start)
    hit = (
        jnp.broadcast_to(in_band, (groups, nets))
        & (first_x < group_at + group_cols)
        & (last_x >= group_at)
    )
    hit = jnp.where(hit, 1.0, 0.0)
    chunks = nets // LANES
    stacked = jnp.concatenate(
        [hit[:, k * LANES : (k + 1) * LANES] for k in range(chunks)], axis=0
    ).astype(BF16)
    below = (iota((LANES, LANES), 0) < iota((LANES, LANES), 1)).astype(F32).astype(BF16)
    before = contract(stacked, below, 1, 0)
    whole = contract(stacked, jnp.ones((LANES, LANES), BF16), 1, 0)
    offset = jnp.zeros((groups, LANES), F32)
    ranks = []
    for k in range(chunks):
        rows = slice(k * groups, (k + 1) * groups)
        ranks.append(before[rows] + offset)
        offset = offset + whole[rows]
    rank = jnp.concatenate(ranks, axis=1)
    rank = jnp.where(hit > 0.0, rank - base.astype(F32), -1.0)
    largest = jnp.max(offset, axis=0, keepdims=True)

    slot = iota((SLOTS, nets), 0).astype(F32)
    field = iota((8, SLOTS), 0)
    for group in range(groups):
        chosen = jnp.where(slot == rank[group : group + 1, :], 1.0, 0.0).astype(BF16)
        got = contract(vals, chosen, 1, 1)
        row = got[0:8] * 256.0 + got[8:16]
        row = jnp.where(field == 5, jnp.broadcast_to(largest, (8, SLOTS)), row)
        for peer in range(group * (peers // groups), (group + 1) * (peers // groups)):
            out_ref[peer] = row


def cells_kernel(tile_rows, tile_cols, bins_ref, area_ref, below_ref, sums_ref):
    cells = bins_ref.shape[1]
    bin_row = lax.shift_right_logical(bins_ref[...], 7)
    bin_col = bins_ref[...] & 127
    area = area_ref[...]
    reach = jnp.where(iota((tile_rows, cells), 0) <= bin_row, 1.0, 0.0).astype(BF16)
    is_col = iota((tile_cols, cells), 0) == bin_col
    pieces = jnp.concatenate(
        [jnp.where(is_col, part.astype(F32), 0.0).astype(BF16) for part in three_parts(area)],
        axis=0,
    )
    below = contract(reach, pieces, 1, 1)
    below = (
        below[:, :tile_cols] + below[:, tile_cols : 2 * tile_cols] + below[:, 2 * tile_cols :]
    )
    below_ref[...] = below
    area_sum = lane_sums(area)
    at = iota((8, LANES), 0)
    sums_ref[...] = jnp.where(
        at == 0,
        jnp.broadcast_to(below[0:1], (8, LANES)),
        jnp.broadcast_to(area_sum, (8, LANES)),
    )


def lane_sums(row):
    total = row[:, :LANES]
    for k in range(1, row.shape[1] // LANES):
        total = total + row[:, k * LANES : (k + 1) * LANES]
    return total


def tile_kernel(
    row_peers,
    has_past,
    row_ref,
    col_ref,
    nets_ref,
    capacity_ref,
    below_ref,
    sums_ref,
    *refs,
):
    if has_past:
        past_ref, *refs = refs
    rudy_ref, excess_ref, pay_ref, hits_ref, cols_ref = refs
    tile_rows, tile_cols = capacity_ref.shape
    row_start = row_ref[0]
    col_start = col_ref[0]
    peers = nets_ref.shape[0]
    row_at = (iota((tile_rows, SLOTS), 0) + row_start).astype(F32)
    col_at = (iota((tile_cols, SLOTS), 0) + col_start).astype(F32)
    largest = jnp.zeros((1, SLOTS), F32)
    for peer in range(peers):
        box = nets_ref[peer]
        first_x, last_x = box[0:1], box[1:2]
        first_y, last_y = box[2:3], box[3:4]
        weight = box[4:5]
        largest = jnp.maximum(largest, box[5:6])
        at = slice(peer * SLOTS, (peer + 1) * SLOTS)
        hits_ref[:, at] = jnp.where(
            (row_at >= first_y) & (row_at <= last_y), 1.0, 0.0
        ).astype(BF16)
        cols_ref[:, at] = jnp.where(
            (col_at >= first_x) & (col_at <= last_x),
            jnp.broadcast_to(weight, col_at.shape),
            0.0,
        ).astype(BF16)
    rudy = contract(hits_ref[...], cols_ref[...], 1, 1)
    if has_past:
        rudy = rudy + past_ref[...]
    rudy_ref[...] = rudy
    excess = jnp.maximum(rudy - capacity_ref[...], 0.0)
    excess_ref[...] = excess
    col_sum = jnp.sum(excess, axis=0, keepdims=True)
    weighed = jnp.sum(excess * below_ref[...], axis=0, keepdims=True)
    at = iota((8, LANES), 0)
    pay = jnp.zeros((8, LANES), F32)
    for k, row in enumerate((col_sum, sums_ref[0:1], sums_ref[1:2], weighed, largest)):
        pay = jnp.where(at == k, jnp.broadcast_to(row, (8, LANES)), pay)
    for peer in range(row_peers):
        pay_ref[peer] = pay


def lookup_kernel(excess_ref, bins_ref, within_ref, looked_ref):
    tile_rows, tile_cols = excess_ref.shape
    half = 256
    lower = (iota((half, half), 0) >= iota((half, half), 1)).astype(F32).astype(BF16)
    carry = jnp.zeros((1, tile_cols), F32)
    parts = []
    for start in range(0, tile_rows, half):
        pieces = jnp.concatenate(three_parts(excess_ref[start : start + half]), axis=1)
        sums = contract(lower, pieces, 1, 0)
        part = (
            sums[:, :tile_cols]
            + sums[:, tile_cols : 2 * tile_cols]
            + sums[:, 2 * tile_cols :]
            + carry
        )
        parts.append(part)
        carry = part[half - 1 : half, :]
    within = jnp.concatenate(parts, axis=0)
    within_ref[...] = within

    cells = bins_ref.shape[1]
    bin_row = lax.shift_right_logical(bins_ref[...], 7)
    bin_col = bins_ref[...] & 127
    row_hot = jnp.where(iota((tile_rows, cells), 0) == bin_row, 1.0, 0.0).astype(BF16)
    turned = jnp.concatenate(three_parts(within.T), axis=0)
    picked = contract(turned, row_hot, 1, 0)
    picked = (
        picked[:tile_cols] + picked[tile_cols : 2 * tile_cols] + picked[2 * tile_cols :]
    )
    is_col = iota((tile_cols, cells), 0) == bin_col
    looked_ref[...] = jnp.sum(jnp.where(is_col, picked, 0.0), axis=0, keepdims=True)


def carry_kernel(factor, me_ref, base_ref, pays_ref, carried_ref, totals_ref, base_out, left_ref):
    me = me_ref[0]
    running = jnp.zeros((1, LANES), F32)
    mine = jnp.zeros((1, LANES), F32)
    area_sum = jnp.zeros((1, LANES), F32)
    weighed = jnp.zeros((1, LANES), F32)
    largest = jnp.zeros((1, LANES), F32)
    for peer in range(pays_ref.shape[0]):
        pay = pays_ref[peer]
        mine = jnp.where(me == peer, running, mine)
        area_sum = area_sum + pay[2:3]
        weighed = weighed + pay[3:4] + pay[1:2] * running
        largest = jnp.maximum(largest, pay[4:5])
        running = running + pay[0:1]
    base_out[0] = base_ref[0] + SLOTS
    left_ref[0] = jnp.max(largest).astype(jnp.int32) - (base_ref[0] + SLOTS)
    carried_ref[...] = jnp.broadcast_to(mine, carried_ref.shape)
    grown = area_sum + factor * weighed
    half = LANES // 2
    both = jnp.where(
        iota((1, LANES), 1) < half,
        area_sum + pltpu.roll(area_sum, half, 1),
        grown + pltpu.roll(grown, half, 1),
    )
    totals_ref[...] = jnp.broadcast_to(both, totals_ref.shape)


def inflation_kernel(factor, within_ref, carried_ref, inflation_ref):
    inflation_ref[...] = 1.0 + factor * (within_ref[...] + carried_ref[0:1])


def sizes_kernel(factor, carried_ref, totals_ref, bins_ref, area_ref, looked_ref, sizes_ref):
    totals = jnp.sum(totals_ref[...], axis=0, keepdims=True)
    lower = iota(totals.shape, 1) < LANES // 2
    area_total = jnp.sum(jnp.where(lower, totals, 0.0), axis=1, keepdims=True)
    grown_total = jnp.sum(jnp.where(lower, 0.0, totals), axis=1, keepdims=True)
    bin_col = bins_ref[...] & 127
    above = jnp.take_along_axis(
        jnp.broadcast_to(carried_ref[0:1], bin_col.shape), bin_col, axis=1
    )
    grown = area_ref[...] * (1.0 + factor * (looked_ref[...] + above))
    sizes_ref[...] = grown * (area_total / grown_total)


def call(kernel, outs, args, scratch=(), limit=16, flops=1_000_000):
    smem = pl.BlockSpec(memory_space=pltpu.SMEM)
    vmem = pl.BlockSpec(memory_space=pltpu.VMEM)
    outs = [o if isinstance(o, jax.ShapeDtypeStruct) else jax.ShapeDtypeStruct(o, F32) for o in outs]
    return pl.pallas_call(
        kernel,
        out_shape=outs,
        in_specs=[smem if a.ndim == 1 else vmem for a in args],
        out_specs=[smem if len(o.shape) == 1 else vmem for o in outs],
        scratch_shapes=list(scratch),
        compiler_params=pltpu.CompilerParams(vmem_limit_bytes=limit * 1024 * 1024),
        cost_estimate=pl.CostEstimate(flops=flops, bytes_accessed=1_000_000, transcendentals=0),
    )(*args)


def exchange(payload, axis):
    return lax.all_to_all(payload, axis, 0, 0, tiled=True)


def per_device(boxes, pins, capacity, cell_bin, cell_area):
    tile_rows, tile_cols = capacity.shape
    rows, cols = lax.axis_size(ROW), lax.axis_size(COL)
    groups = lax.axis_size("col_0")
    nets = boxes.shape[1]
    cells = cell_bin.shape[1]
    factor = 2.0 / (tile_rows * rows)
    row_at = lax.axis_index(ROW)[None]
    row_start = row_at * tile_rows
    col_start = lax.axis_index(COL)[None] * tile_cols
    pins = pins.reshape(1, nets)
    below, cell_sums = call(
        functools.partial(cells_kernel, tile_rows, tile_cols),
        [(tile_rows, tile_cols), (8, LANES)],
        (cell_bin, cell_area),
        flops=4_000_000_000,
    )

    def one_round(base, past):
        (packed,) = call(
            functools.partial(
                pack_kernel, cols, groups, tile_cols * (cols // groups), tile_rows
            ),
            [(cols, 8, SLOTS)],
            (row_start, base, boxes, pins),
            [pltpu.VMEM((16, nets), F32)],
        )
        mine = exchange(packed, COL)
        rudy, excess, pay = call(
            functools.partial(tile_kernel, rows, past is not None),
            [(tile_rows, tile_cols), (tile_rows, tile_cols), (rows, 8, LANES)],
            (row_start, col_start, mine, capacity, below, cell_sums)
            + (() if past is None else (past,)),
            [
                pltpu.VMEM((tile_rows, cols * SLOTS), BF16),
                pltpu.VMEM((tile_cols, cols * SLOTS), BF16),
            ],
            limit=28,
        )
        pays = exchange(pay, ROW)
        within, looked = call(
            lookup_kernel,
            [(tile_rows, tile_cols), (1, cells)],
            (excess, cell_bin),
            limit=28,
            flops=4_000_000_000,
        )
        one = jax.ShapeDtypeStruct((1,), jnp.int32)
        carried, totals, base, left = call(
            functools.partial(carry_kernel, factor),
            [(8, LANES), (cols, LANES), one, one],
            (row_at, base, pays),
        )
        return left, base, rudy, within, looked, carried, totals

    def unfinished(state):
        return state[0][0] > 0

    def next_round(state):
        return one_round(state[1], state[2])

    first = one_round(jnp.zeros((1,), jnp.int32), None)
    _, _, rudy, within, looked, carried, totals = lax.while_loop(unfinished, next_round, first)

    totals = exchange(totals, COL)
    shape = (cells // LANES, LANES)
    (inflation,) = call(
        functools.partial(inflation_kernel, factor),
        [(tile_rows, tile_cols)],
        (within, carried),
        flops=4_000_000_000,
    )
    (sizes,) = call(
        functools.partial(sizes_kernel, factor),
        [shape],
        (carried, totals, cell_bin.reshape(shape), cell_area.reshape(shape), looked.reshape(shape)),
    )
    return rudy, inflation, sizes.reshape(cell_area.shape)


def solution(mesh):
    split = Mesh(mesh.devices.reshape(4, 2, 8, 2, 2), ROW + COL)
    placed = (P(None, COL), P(COL), P(ROW, COL), P(ROW, COL), P(ROW, COL))
    return jax.shard_map(
        per_device,
        mesh=split,
        in_specs=placed,
        out_specs=(P(ROW, COL), P(ROW, COL), P(ROW, COL)),
        check_vma=False,
    )
```

```python
import functools

import jax
import jax.numpy as jnp
from jax import lax
from jax.experimental import pallas as pl
from jax.experimental.pallas import tpu as pltpu
from jax.sharding import Mesh
from jax.sharding import PartitionSpec as P

ROW = ("row_0", "row_1")
COL = ("col_0", "col_1", "col_2")
NEAR = ("row_0", "row_1", "col_1", "col_2")
SLOTS = 128
LANES = 128
F32 = jnp.float32
BF16 = jnp.bfloat16


def iota(shape, dim):
    return lax.broadcasted_iota(jnp.int32, shape, dim)


def contract(a, b, dim_a, dim_b):
    return lax.dot_general(
        a, b, (((dim_a,), (dim_b,)), ((), ())), preferred_element_type=F32
    )


def three_parts(x):
    high = x.astype(BF16)
    rest = x - high.astype(F32)
    middle = rest.astype(BF16)
    low = (rest - middle.astype(F32)).astype(BF16)
    return high, middle, low


def pack_kernel(
    peers, groups, group_cols, tile_rows, row_ref, base_ref, boxes_ref, pins_ref, out_ref, vals_ref
):
    nets = boxes_ref.shape[1]
    row_start = row_ref[0]
    base = base_ref[0]
    first_x, last_x = boxes_ref[0:1, :], boxes_ref[1:2, :]
    first_y, last_y = boxes_ref[2:3, :], boxes_ref[3:4, :]
    span_x = (last_x - first_x + 1).astype(F32)
    span_y = (last_y - first_y + 1).astype(F32)
    weight = jnp.log(pins_ref[...].astype(F32)) * (span_x + span_y) / (span_x * span_y)
    weight = weight.astype(BF16).astype(F32)
    vals_ref[...] = jnp.zeros_like(vals_ref)
    vals_ref[0:4, :] = lax.shift_right_logical(boxes_ref[...], 8).astype(F32)
    vals_ref[4:5, :] = weight * (1.0 / 256.0)
    vals_ref[8:12, :] = (boxes_ref[...] & 255).astype(F32)
    vals = vals_ref[...].astype(BF16)

    group_at = iota((groups, nets), 0) * group_cols
    in_band = (first_y < row_start + tile_rows) & (last_y >= row_start)
    hit = (
        jnp.broadcast_to(in_band, (groups, nets))
        & (first_x < group_at + group_cols)
        & (last_x >= group_at)
    )
    hit = jnp.where(hit, 1.0, 0.0)
    chunks = nets // LANES
    stacked = jnp.concatenate(
        [hit[:, k * LANES : (k + 1) * LANES] for k in range(chunks)], axis=0
    ).astype(BF16)
    below = (iota((LANES, LANES), 0) < iota((LANES, LANES), 1)).astype(F32).astype(BF16)
    before = contract(stacked, below, 1, 0)
    whole = contract(stacked, jnp.ones((LANES, LANES), BF16), 1, 0)
    offset = jnp.zeros((groups, LANES), F32)
    ranks = []
    for k in range(chunks):
        rows = slice(k * groups, (k + 1) * groups)
        ranks.append(before[rows] + offset)
        offset = offset + whole[rows]
    rank = jnp.concatenate(ranks, axis=1)
    rank = jnp.clip(rank - base.astype(F32), -1.0, float(SLOTS))
    rank = jnp.where(hit > 0.0, rank, -1.0)
    largest = jnp.max(offset, axis=0, keepdims=True)

    slot = iota((SLOTS, nets), 0).astype(F32).astype(BF16)
    field = iota((8, SLOTS), 0)
    for group in range(groups):
        mine = jnp.broadcast_to(rank[group : group + 1, :], (16, nets)).astype(BF16)
        mine = jnp.concatenate([mine] * (SLOTS // 16), axis=0)
        chosen = jnp.where(slot == mine, BF16(1), BF16(0))
        got = contract(vals, chosen, 1, 1)
        row = got[0:8] * 256.0 + got[8:16]
        row = jnp.where(field == 5, jnp.broadcast_to(largest, (8, SLOTS)), row)
        for peer in range(group * (peers // groups), (group + 1) * (peers // groups)):
            out_ref[peer] = row


def cells_kernel(tile_rows, tile_cols, bins_ref, area_ref, below_ref, sums_ref):
    cells = bins_ref.shape[1]
    bin_row = lax.shift_right_logical(bins_ref[...], 7)
    bin_col = bins_ref[...] & 127
    area = area_ref[...]
    reach = jnp.where(iota((tile_rows, cells), 0) <= bin_row, 1.0, 0.0).astype(BF16)
    is_col = iota((tile_cols, cells), 0) == bin_col
    pieces = jnp.concatenate(
        [jnp.where(is_col, part.astype(F32), 0.0).astype(BF16) for part in three_parts(area)],
        axis=0,
    )
    below = contract(reach, pieces, 1, 1)
    below = (
        below[:, :tile_cols] + below[:, tile_cols : 2 * tile_cols] + below[:, 2 * tile_cols :]
    )
    below_ref[...] = below
    area_sum = lane_sums(area)
    at = iota((8, LANES), 0)
    sums_ref[...] = jnp.where(
        at == 0,
        jnp.broadcast_to(below[0:1], (8, LANES)),
        jnp.broadcast_to(area_sum, (8, LANES)),
    )


def lane_sums(row):
    total = row[:, :LANES]
    for k in range(1, row.shape[1] // LANES):
        total = total + row[:, k * LANES : (k + 1) * LANES]
    return total


def tall(row, rows):
    short = jnp.broadcast_to(row, (16, row.shape[1])).astype(BF16)
    return jnp.concatenate([short] * (rows // 16), axis=0)


def inside(first, last, start, count):
    first = jnp.clip(first - start, 0.0, float(count))
    last = jnp.clip(last - start, -1.0, float(count - 1))
    return tall(first, count), tall(last, count)


def tile_kernel(
    has_past,
    row_ref,
    col_ref,
    nets_ref,
    capacity_ref,
    below_ref,
    sums_ref,
    *refs,
):
    if has_past:
        past_ref, *refs = refs
    rudy_ref, excess_ref, pay_ref = refs
    tile_rows, tile_cols = capacity_ref.shape
    row_start = row_ref[0]
    col_start = col_ref[0]
    peers = nets_ref.shape[0]
    half = 256
    at = iota((half, SLOTS), 0).astype(F32).astype(BF16)
    col_at = at[:tile_cols]
    largest = jnp.zeros((1, SLOTS), F32)
    starts = [col_start.astype(F32)] + [
        (row_start + first).astype(F32) for first in range(0, tile_rows, half)
    ]
    rudy = jnp.zeros((tile_rows, tile_cols), F32)
    step = 4
    for peer in range(0, peers, step):
        hits, cols = [], []
        for box in [nets_ref[peer + k] for k in range(step)]:
            largest = jnp.maximum(largest, box[5:6])
            hit = []
            for first in starts[1:]:
                low, high = inside(box[2:3], box[3:4], first, half)
                hit.append(
                    jnp.where((at >= low) & (at <= high), BF16(1), BF16(0))
                )
            hits.append(jnp.concatenate(hit, axis=0))
            low, high = inside(box[0:1], box[1:2], starts[0], tile_cols)
            weight = tall(box[4:5], tile_cols)
            cols.append(jnp.where((col_at >= low) & (col_at <= high), weight, BF16(0)))
        rudy = rudy + contract(
            jnp.concatenate(hits, axis=1), jnp.concatenate(cols, axis=1), 1, 1
        )
    if has_past:
        rudy = rudy + past_ref[...]
    rudy_ref[...] = rudy
    excess = jnp.maximum(rudy - capacity_ref[...], 0.0)
    excess_ref[...] = excess
    col_sum = jnp.sum(excess, axis=0, keepdims=True)
    weighed = jnp.sum(excess * below_ref[...], axis=0, keepdims=True)
    at = iota((8, LANES), 0) & 3
    shared = halves(sums_ref[1:2], weighed)
    pay = jnp.broadcast_to(largest, (8, LANES))
    for k, row in enumerate((col_sum, sums_ref[0:1], shared)):
        pay = jnp.where(at == k, jnp.broadcast_to(row, (8, LANES)), pay)
    for k in range(pay_ref.shape[0] // 8):
        pay_ref[8 * k : 8 * k + 8] = pay


def halves(a, b):
    half = LANES // 2
    lower = iota((1, LANES), 1) < half
    return jnp.where(lower, a + pltpu.roll(a, half, 1), b + pltpu.roll(b, half, 1))


def lookup_kernel(excess_ref, bins_ref, within_ref, looked_ref):
    tile_rows, tile_cols = excess_ref.shape
    half = 256
    lower = (iota((half, half), 0) >= iota((half, half), 1)).astype(F32).astype(BF16)
    carry = jnp.zeros((1, tile_cols), F32)
    parts = []
    for start in range(0, tile_rows, half):
        pieces = jnp.concatenate(three_parts(excess_ref[start : start + half]), axis=1)
        sums = contract(lower, pieces, 1, 0)
        part = (
            sums[:, :tile_cols]
            + sums[:, tile_cols : 2 * tile_cols]
            + sums[:, 2 * tile_cols :]
            + carry
        )
        parts.append(part)
        carry = part[half - 1 : half, :]
    within = jnp.concatenate(parts, axis=0)
    within_ref[...] = within

    cells = bins_ref.shape[1]
    bin_row = lax.shift_right_logical(bins_ref[...], 7)
    bin_col = bins_ref[...] & 127
    row_hot = jnp.where(iota((tile_rows, cells), 0) == bin_row, 1.0, 0.0).astype(BF16)
    turned = jnp.concatenate(three_parts(within.T), axis=0)
    picked = contract(turned, row_hot, 1, 0)
    picked = (
        picked[:tile_cols] + picked[tile_cols : 2 * tile_cols] + picked[2 * tile_cols :]
    )
    is_col = iota((tile_cols, cells), 0) == bin_col
    looked_ref[...] = jnp.sum(jnp.where(is_col, picked, 0.0), axis=0, keepdims=True)


def carry_kernel(
    rows, factor, row_ref, col_ref, base_ref, pays_ref, carried_ref, totals_ref, base_out, left_ref
):
    row_me, col_me = row_ref[0], col_ref[0]
    width = pays_ref.shape[0] // (4 * rows)
    mine = jnp.zeros((1, LANES), F32)
    bilinear = jnp.zeros((1, LANES), F32)
    shared = jnp.zeros((1, LANES), F32)
    largest = jnp.zeros((1, LANES), F32)
    for col in range(width):
        running = jnp.zeros((1, LANES), F32)
        for row in range(rows):
            at = 4 * (row * width + col)
            pay = pays_ref[at : at + 4]
            mine = jnp.where((row_me == row) & (col_me == col), running, mine)
            bilinear = bilinear + pay[1:2] * running
            shared = shared + pay[2:3]
            largest = jnp.maximum(largest, pay[3:4])
            running = running + pay[0:1]
    base_out[0] = base_ref[0] + SLOTS
    left_ref[0] = jnp.max(largest).astype(jnp.int32) - (base_ref[0] + SLOTS)
    carried_ref[...] = jnp.broadcast_to(mine, carried_ref.shape)
    totals = shared + halves(jnp.zeros((1, LANES), F32), bilinear)
    totals_ref[...] = jnp.broadcast_to(totals, totals_ref.shape)


def inflation_kernel(factor, within_ref, carried_ref, inflation_ref):
    inflation_ref[...] = 1.0 + factor * (within_ref[...] + carried_ref[0:1])


def sizes_kernel(factor, carried_ref, totals_ref, bins_ref, area_ref, looked_ref, sizes_ref):
    totals = jnp.sum(totals_ref[...], axis=0, keepdims=True)
    lower = iota(totals.shape, 1) < LANES // 2
    area_total = jnp.sum(jnp.where(lower, totals, 0.0), axis=1, keepdims=True)
    added = jnp.sum(jnp.where(lower, 0.0, totals), axis=1, keepdims=True)
    grown_total = area_total + factor * added
    bin_col = bins_ref[...] & 127
    above = jnp.take_along_axis(
        jnp.broadcast_to(carried_ref[0:1], bin_col.shape), bin_col, axis=1
    )
    grown = area_ref[...] * (1.0 + factor * (looked_ref[...] + above))
    sizes_ref[...] = grown * (area_total / grown_total)


def call(kernel, outs, args, scratch=(), limit=16, flops=1_000_000):
    smem = pl.BlockSpec(memory_space=pltpu.SMEM)
    vmem = pl.BlockSpec(memory_space=pltpu.VMEM)
    outs = [o if isinstance(o, jax.ShapeDtypeStruct) else jax.ShapeDtypeStruct(o, F32) for o in outs]
    return pl.pallas_call(
        kernel,
        out_shape=outs,
        in_specs=[smem if a.ndim == 1 else vmem for a in args],
        out_specs=[smem if len(o.shape) == 1 else vmem for o in outs],
        scratch_shapes=list(scratch),
        compiler_params=pltpu.CompilerParams(vmem_limit_bytes=limit * 1024 * 1024),
        cost_estimate=pl.CostEstimate(flops=flops, bytes_accessed=1_000_000, transcendentals=0),
    )(*args)


def exchange(payload, axis):
    return lax.all_to_all(payload, axis, 0, 0, tiled=True)


def per_device(boxes, pins, capacity, cell_bin, cell_area):
    tile_rows, tile_cols = capacity.shape
    rows, cols = lax.axis_size(ROW), lax.axis_size(COL)
    groups = lax.axis_size("col_0")
    nets = boxes.shape[1]
    cells = cell_bin.shape[1]
    factor = 2.0 / (tile_rows * rows)
    row_at = lax.axis_index(ROW)[None]
    near = lax.axis_size(NEAR)
    near_at = lax.axis_index(("col_1", "col_2"))[None]
    row_start = row_at * tile_rows
    col_start = lax.axis_index(COL)[None] * tile_cols
    pins = pins.reshape(1, nets)
    below, cell_sums = call(
        functools.partial(cells_kernel, tile_rows, tile_cols),
        [(tile_rows, tile_cols), (8, LANES)],
        (cell_bin, cell_area),
        flops=4_000_000_000,
    )

    def one_round(base, past):
        (packed,) = call(
            functools.partial(
                pack_kernel, cols, groups, tile_cols * (cols // groups), tile_rows
            ),
            [(cols, 8, SLOTS)],
            (row_start, base, boxes, pins),
            [pltpu.VMEM((16, nets), F32)],
        )
        mine = exchange(packed, COL)
        rudy, excess, pay = call(
            functools.partial(tile_kernel, past is not None),
            [(tile_rows, tile_cols), (tile_rows, tile_cols), (near * 4, LANES)],
            (row_start, col_start, mine, capacity, below, cell_sums)
            + (() if past is None else (past,)),
            limit=28,
        )
        pays = exchange(pay.reshape(near, 4, LANES), NEAR).reshape(near * 4, LANES)
        within, looked = call(
            lookup_kernel,
            [(tile_rows, tile_cols), (1, cells)],
            (excess, cell_bin),
            limit=28,
            flops=4_000_000_000,
        )
        one = jax.ShapeDtypeStruct((1,), jnp.int32)
        carried, totals, base, left = call(
            functools.partial(carry_kernel, rows, factor),
            [(8, LANES), (groups, LANES), one, one],
            (row_at, near_at, base, pays),
        )
        return left, base, rudy, within, looked, carried, totals

    def unfinished(state):
        return state[0][0] > 0

    def next_round(state):
        return one_round(state[1], state[2])

    first = one_round(jnp.zeros((1,), jnp.int32), None)
    _, _, rudy, within, looked, carried, totals = lax.while_loop(unfinished, next_round, first)

    totals = exchange(totals, "col_0")
    shape = (cells // LANES, LANES)
    (inflation,) = call(
        functools.partial(inflation_kernel, factor),
        [(tile_rows, tile_cols)],
        (within, carried),
        flops=4_000_000_000,
    )
    (sizes,) = call(
        functools.partial(sizes_kernel, factor),
        [shape],
        (carried, totals, cell_bin.reshape(shape), cell_area.reshape(shape), looked.reshape(shape)),
    )
    return rudy, inflation, sizes.reshape(cell_area.shape)


def solution(mesh):
    split = Mesh(mesh.devices.reshape(4, 2, 8, 2, 2), ROW + COL)
    placed = (P(None, COL), P(COL), P(ROW, COL), P(ROW, COL), P(ROW, COL))
    return jax.shard_map(
        per_device,
        mesh=split,
        in_specs=placed,
        out_specs=(P(ROW, COL), P(ROW, COL), P(ROW, COL)),
        check_vma=False,
    )
```

```python
import functools

import jax
import jax.numpy as jnp
from jax import lax
from jax.experimental import pallas as pl
from jax.experimental.pallas import tpu as pltpu
from jax.sharding import Mesh
from jax.sharding import PartitionSpec as P

ROW = ("row_0", "row_1")
COL = ("col_0", "col_1", "col_2")
NEAR = ("row_0", "row_1", "col_1", "col_2")
SLOTS = 128
LANES = 128
F32 = jnp.float32
BF16 = jnp.bfloat16


def iota(shape, dim):
    return lax.broadcasted_iota(jnp.int32, shape, dim)


def contract(a, b, dim_a, dim_b):
    return lax.dot_general(
        a, b, (((dim_a,), (dim_b,)), ((), ())), preferred_element_type=F32
    )


def three_parts(x):
    high = x.astype(BF16)
    rest = x - high.astype(F32)
    middle = rest.astype(BF16)
    low = (rest - middle.astype(F32)).astype(BF16)
    return high, middle, low


def pack_kernel(
    peers, groups, group_cols, tile_rows, boxes_ref, pins_ref, *refs
):
    nets = boxes_ref.shape[1]
    *base_ref, out_ref, vals_ref = refs
    base = base_ref[0][0] if base_ref else jnp.int32(0)
    row_start = lax.axis_index(ROW) * tile_rows
    first_x, last_x = boxes_ref[0:1, :], boxes_ref[1:2, :]
    first_y, last_y = boxes_ref[2:3, :], boxes_ref[3:4, :]
    span_x = (last_x - first_x + 1).astype(F32)
    span_y = (last_y - first_y + 1).astype(F32)
    weight = jnp.log(pins_ref[...].astype(F32)) * (span_x + span_y) / (span_x * span_y)
    weight = weight.astype(BF16).astype(F32)
    vals_ref[...] = jnp.zeros_like(vals_ref)
    vals_ref[0:4, :] = lax.shift_right_logical(boxes_ref[...], 8).astype(F32)
    vals_ref[4:5, :] = weight * (1.0 / 256.0)
    vals_ref[8:12, :] = (boxes_ref[...] & 255).astype(F32)
    vals = vals_ref[...].astype(BF16)

    group_at = iota((groups, nets), 0) * group_cols
    in_band = (first_y < row_start + tile_rows) & (last_y >= row_start)
    hit = (
        jnp.broadcast_to(in_band, (groups, nets))
        & (first_x < group_at + group_cols)
        & (last_x >= group_at)
    )
    hit = jnp.where(hit, 1.0, 0.0)
    chunks = nets // LANES
    stacked = jnp.concatenate(
        [hit[:, k * LANES : (k + 1) * LANES] for k in range(chunks)], axis=0
    ).astype(BF16)
    below = (iota((LANES, LANES), 0) < iota((LANES, LANES), 1)).astype(F32).astype(BF16)
    before = contract(stacked, below, 1, 0)
    whole = contract(stacked, jnp.ones((LANES, LANES), BF16), 1, 0)
    offset = jnp.zeros((groups, LANES), F32)
    ranks = []
    for k in range(chunks):
        rows = slice(k * groups, (k + 1) * groups)
        ranks.append(before[rows] + offset)
        offset = offset + whole[rows]
    rank = jnp.concatenate(ranks, axis=1)
    rank = jnp.clip(rank - base.astype(F32), -1.0, float(SLOTS))
    rank = jnp.where(hit > 0.0, rank, -1.0)
    largest = jnp.max(offset, axis=0, keepdims=True)

    slot = iota((SLOTS, nets), 0).astype(F32).astype(BF16)
    field = iota((8, SLOTS), 0)
    for group in range(groups):
        mine = jnp.broadcast_to(rank[group : group + 1, :], (16, nets)).astype(BF16)
        mine = jnp.concatenate([mine] * (SLOTS // 16), axis=0)
        chosen = jnp.where(slot == mine, BF16(1), BF16(0))
        got = contract(vals, chosen, 1, 1)
        row = got[0:8] * 256.0 + got[8:16]
        row = jnp.where(field == 5, jnp.broadcast_to(largest, (8, SLOTS)), row)
        for peer in range(group * (peers // groups), (group + 1) * (peers // groups)):
            out_ref[peer] = row


def cells_kernel(tile_rows, tile_cols, bins_ref, area_ref, below_ref, sums_ref):
    cells = bins_ref.shape[1]
    bin_row = lax.shift_right_logical(bins_ref[...], 7)
    bin_col = bins_ref[...] & 127
    area = area_ref[...]
    reach = jnp.where(iota((tile_rows, cells), 0) <= bin_row, 1.0, 0.0).astype(BF16)
    is_col = iota((tile_cols, cells), 0) == bin_col
    pieces = jnp.concatenate(
        [jnp.where(is_col, part.astype(F32), 0.0).astype(BF16) for part in three_parts(area)],
        axis=0,
    )
    below = contract(reach, pieces, 1, 1)
    below = (
        below[:, :tile_cols] + below[:, tile_cols : 2 * tile_cols] + below[:, 2 * tile_cols :]
    )
    below_ref[...] = below
    area_sum = lane_sums(area)
    at = iota((8, LANES), 0)
    sums_ref[...] = jnp.where(
        at == 0,
        jnp.broadcast_to(below[0:1], (8, LANES)),
        jnp.broadcast_to(area_sum, (8, LANES)),
    )


def lane_sums(row):
    total = row[:, :LANES]
    for k in range(1, row.shape[1] // LANES):
        total = total + row[:, k * LANES : (k + 1) * LANES]
    return total


def tall(row, rows):
    short = jnp.broadcast_to(row, (16, row.shape[1])).astype(BF16)
    return jnp.concatenate([short] * (rows // 16), axis=0)


def inside(first, last, start, count):
    first = jnp.clip(first - start, 0.0, float(count))
    last = jnp.clip(last - start, -1.0, float(count - 1))
    return tall(first, count), tall(last, count)


def tile_kernel(
    has_past,
    nets_ref,
    capacity_ref,
    below_ref,
    sums_ref,
    *refs,
):
    if has_past:
        past_ref, *refs = refs
    rudy_ref, pay_ref = refs
    tile_rows, tile_cols = capacity_ref.shape
    row_start = lax.axis_index(ROW) * tile_rows
    col_start = lax.axis_index(COL) * tile_cols
    peers = nets_ref.shape[0]
    half = 256
    at = iota((half, SLOTS), 0).astype(F32).astype(BF16)
    col_at = at[:tile_cols]
    largest = jnp.zeros((1, SLOTS), F32)
    starts = [col_start.astype(F32)] + [
        (row_start + first).astype(F32) for first in range(0, tile_rows, half)
    ]
    rudy = jnp.zeros((tile_rows, tile_cols), F32)
    step = 4
    for peer in range(0, peers, step):
        hits, cols = [], []
        for box in [nets_ref[peer + k] for k in range(step)]:
            largest = jnp.maximum(largest, box[5:6])
            hit = []
            for first in starts[1:]:
                low, high = inside(box[2:3], box[3:4], first, half)
                hit.append(
                    jnp.where((at >= low) & (at <= high), BF16(1), BF16(0))
                )
            hits.append(jnp.concatenate(hit, axis=0))
            low, high = inside(box[0:1], box[1:2], starts[0], tile_cols)
            weight = tall(box[4:5], tile_cols)
            cols.append(jnp.where((col_at >= low) & (col_at <= high), weight, BF16(0)))
        rudy = rudy + contract(
            jnp.concatenate(hits, axis=1), jnp.concatenate(cols, axis=1), 1, 1
        )
    if has_past:
        rudy = rudy + past_ref[...]
    rudy_ref[...] = rudy
    excess = jnp.maximum(rudy - capacity_ref[...], 0.0)
    col_sum = jnp.sum(excess, axis=0, keepdims=True)
    weighed = jnp.sum(excess * below_ref[...], axis=0, keepdims=True)
    at = iota((8, LANES), 0) & 3
    shared = halves(sums_ref[1:2], weighed)
    pay = jnp.broadcast_to(largest, (8, LANES))
    for k, row in enumerate((col_sum, sums_ref[0:1], shared)):
        pay = jnp.where(at == k, jnp.broadcast_to(row, (8, LANES)), pay)
    for k in range(pay_ref.shape[0] // 8):
        pay_ref[8 * k : 8 * k + 8] = pay


def halves(a, b):
    half = LANES // 2
    lower = iota((1, LANES), 1) < half
    return jnp.where(lower, a + pltpu.roll(a, half, 1), b + pltpu.roll(b, half, 1))


def inflation_kernel(
    factor, rudy_ref, capacity_ref, bins_ref, carried_ref, inflation_ref, looked_ref
):
    tile_rows, tile_cols = rudy_ref.shape
    excess = jnp.maximum(rudy_ref[...] - capacity_ref[...], 0.0)
    half = 256
    lower = (iota((half, half), 0) >= iota((half, half), 1)).astype(F32).astype(BF16)
    carry = jnp.zeros((1, tile_cols), F32)
    parts = []
    for start in range(0, tile_rows, half):
        pieces = jnp.concatenate(three_parts(excess[start : start + half]), axis=1)
        sums = contract(lower, pieces, 1, 0)
        part = (
            sums[:, :tile_cols]
            + sums[:, tile_cols : 2 * tile_cols]
            + sums[:, 2 * tile_cols :]
            + carry
        )
        parts.append(part)
        carry = part[half - 1 : half, :]
    within = jnp.concatenate(parts, axis=0)
    inflation_ref[...] = 1.0 + factor * (within + carried_ref[0:1])

    cells = bins_ref.shape[1]
    bin_row = lax.shift_right_logical(bins_ref[...], 7)
    bin_col = bins_ref[...] & 127
    row_hot = jnp.where(iota((tile_rows, cells), 0) == bin_row, 1.0, 0.0).astype(BF16)
    turned = jnp.concatenate(three_parts(within.T), axis=0)
    picked = contract(turned, row_hot, 1, 0)
    picked = (
        picked[:tile_cols] + picked[tile_cols : 2 * tile_cols] + picked[2 * tile_cols :]
    )
    is_col = iota((tile_cols, cells), 0) == bin_col
    looked_ref[...] = jnp.sum(jnp.where(is_col, picked, 0.0), axis=0, keepdims=True)


def carry_kernel(rows, pays_ref, *refs):
    *base_ref, carried_ref, totals_ref, base_out, left_ref = refs
    base = (base_ref[0][0] if base_ref else 0) + SLOTS
    row_me = lax.axis_index(ROW)
    col_me = lax.axis_index(("col_1", "col_2"))
    width = pays_ref.shape[0] // (4 * rows)
    mine = jnp.zeros((1, LANES), F32)
    bilinear = jnp.zeros((1, LANES), F32)
    shared = jnp.zeros((1, LANES), F32)
    largest = jnp.zeros((1, LANES), F32)
    for col in range(width):
        running = jnp.zeros((1, LANES), F32)
        for row in range(rows):
            at = 4 * (row * width + col)
            pay = pays_ref[at : at + 4]
            mine = jnp.where((row_me == row) & (col_me == col), running, mine)
            bilinear = bilinear + pay[1:2] * running
            shared = shared + pay[2:3]
            largest = jnp.maximum(largest, pay[3:4])
            running = running + pay[0:1]
    base_out[0] = jnp.int32(base)
    left_ref[0] = jnp.max(largest).astype(jnp.int32) - base
    carried_ref[...] = jnp.broadcast_to(mine, carried_ref.shape)
    totals = shared + halves(jnp.zeros((1, LANES), F32), bilinear)
    totals_ref[...] = jnp.broadcast_to(totals, totals_ref.shape)


def sizes_kernel(factor, carried_ref, totals_ref, bins_ref, area_ref, looked_ref, sizes_ref):
    totals = jnp.sum(totals_ref[...], axis=0, keepdims=True)
    lower = iota(totals.shape, 1) < LANES // 2
    area_total = jnp.sum(jnp.where(lower, totals, 0.0), axis=1, keepdims=True)
    added = jnp.sum(jnp.where(lower, 0.0, totals), axis=1, keepdims=True)
    grown_total = area_total + factor * added
    bin_col = bins_ref[...] & 127
    above = jnp.take_along_axis(
        jnp.broadcast_to(carried_ref[0:1], bin_col.shape), bin_col, axis=1
    )
    grown = area_ref[...] * (1.0 + factor * (looked_ref[...] + above))
    sizes_ref[...] = grown * (area_total / grown_total)


def call(kernel, outs, args, scratch=(), limit=16, flops=1_000_000):
    smem = pl.BlockSpec(memory_space=pltpu.SMEM)
    vmem = pl.BlockSpec(memory_space=pltpu.VMEM)
    outs = [o if isinstance(o, jax.ShapeDtypeStruct) else jax.ShapeDtypeStruct(o, F32) for o in outs]
    return pl.pallas_call(
        kernel,
        out_shape=outs,
        in_specs=[smem if a.ndim == 1 else vmem for a in args],
        out_specs=[smem if len(o.shape) == 1 else vmem for o in outs],
        scratch_shapes=list(scratch),
        compiler_params=pltpu.CompilerParams(vmem_limit_bytes=limit * 1024 * 1024),
        cost_estimate=pl.CostEstimate(flops=flops, bytes_accessed=1_000_000, transcendentals=0),
    )(*args)


def exchange(payload, axis):
    return lax.all_to_all(payload, axis, 0, 0, tiled=True)


def per_device(boxes, pins, capacity, cell_bin, cell_area):
    tile_rows, tile_cols = capacity.shape
    rows, cols = lax.axis_size(ROW), lax.axis_size(COL)
    groups = lax.axis_size("col_0")
    nets = boxes.shape[1]
    cells = cell_bin.shape[1]
    factor = 2.0 / (tile_rows * rows)
    near = lax.axis_size(NEAR)
    pins = pins.reshape(1, nets)
    below, cell_sums = call(
        functools.partial(cells_kernel, tile_rows, tile_cols),
        [(tile_rows, tile_cols), (8, LANES)],
        (cell_bin, cell_area),
        flops=4_000_000_000,
    )

    def one_round(base, past):
        (packed,) = call(
            functools.partial(
                pack_kernel, cols, groups, tile_cols * (cols // groups), tile_rows
            ),
            [(cols, 8, SLOTS)],
            (boxes, pins) + base,
            [pltpu.VMEM((16, nets), F32)],
        )
        mine = exchange(packed, COL)
        rudy, pay = call(
            functools.partial(tile_kernel, past is not None),
            [(tile_rows, tile_cols), (near * 4, LANES)],
            (mine, capacity, below, cell_sums)
            + (() if past is None else (past,)),
            limit=28,
        )
        pays = exchange(pay.reshape(near, 4, LANES), NEAR).reshape(near * 4, LANES)
        one = jax.ShapeDtypeStruct((1,), jnp.int32)
        carried, totals, reached, left = call(
            functools.partial(carry_kernel, rows),
            [(8, LANES), (groups, LANES), one, one],
            (pays,) + base,
        )
        return left, reached, rudy, carried, totals

    def unfinished(state):
        return state[0][0] > 0

    def next_round(state):
        return one_round((state[1],), state[2])

    first = one_round((), None)
    _, _, rudy, carried, totals = lax.cond(
        unfinished(first),
        lambda state: lax.while_loop(unfinished, next_round, state),
        lambda state: state,
        first,
    )

    totals = exchange(totals, "col_0")
    shape = (cells // LANES, LANES)
    inflation, looked = call(
        functools.partial(inflation_kernel, factor),
        [(tile_rows, tile_cols), (1, cells)],
        (rudy, capacity, cell_bin, carried),
        limit=28,
        flops=4_000_000_000,
    )
    (sizes,) = call(
        functools.partial(sizes_kernel, factor),
        [shape],
        (carried, totals, cell_bin.reshape(shape), cell_area.reshape(shape), looked.reshape(shape)),
    )
    return rudy, inflation, sizes.reshape(cell_area.shape)


def solution(mesh):
    split = Mesh(mesh.devices.reshape(4, 2, 8, 2, 2), ROW + COL)
    placed = (P(None, COL), P(COL), P(ROW, COL), P(ROW, COL), P(ROW, COL))
    return jax.shard_map(
        per_device,
        mesh=split,
        in_specs=placed,
        out_specs=(P(ROW, COL), P(ROW, COL), P(ROW, COL)),
        check_vma=False,
    )
```

```python
import functools
import math

import jax
import jax.numpy as jnp
from jax import lax
from jax.experimental import pallas as pl
from jax.experimental.pallas import tpu as pltpu
from jax.sharding import Mesh
from jax.sharding import PartitionSpec as P

ROW = ("row_0", "row_1")
COL = ("col_0", "col_1", "col_2")
NEAR = ("row_0", "row_1", "col_1", "col_2")
SLOTS = 128
LANES = 128
F32 = jnp.float32
BF16 = jnp.bfloat16


def iota(shape, dim):
    return lax.broadcasted_iota(jnp.int32, shape, dim)


def contract(a, b, dim_a, dim_b):
    return lax.dot_general(
        a, b, (((dim_a,), (dim_b,)), ((), ())), preferred_element_type=F32
    )


def three_parts(x):
    high = x.astype(BF16)
    rest = x - high.astype(F32)
    middle = rest.astype(BF16)
    low = (rest - middle.astype(F32)).astype(BF16)
    return high, middle, low


def pack_kernel(
    order, peers, groups, group_cols, tile_rows, boxes_ref, pins_ref, *refs
):
    nets = boxes_ref.shape[1]
    *base_ref, out_ref, vals_ref = refs
    base = base_ref[0][0] if base_ref else jnp.int32(0)
    row_start = lax.axis_index(ROW) * tile_rows
    first_x, last_x = boxes_ref[0:1, :], boxes_ref[1:2, :]
    first_y, last_y = boxes_ref[2:3, :], boxes_ref[3:4, :]
    span_x = (last_x - first_x + 1).astype(F32)
    span_y = (last_y - first_y + 1).astype(F32)
    weight = jnp.log(pins_ref[...].astype(F32)) * (span_x + span_y) / (span_x * span_y)
    weight = weight.astype(BF16).astype(F32)
    vals_ref[...] = jnp.zeros_like(vals_ref)
    vals_ref[0:4, :] = lax.shift_right_logical(boxes_ref[...], 8).astype(F32)
    vals_ref[4:5, :] = weight * (1.0 / 256.0)
    vals_ref[8:12, :] = (boxes_ref[...] & 255).astype(F32)
    vals = vals_ref[...].astype(BF16)

    group_at = iota((groups, nets), 0) * group_cols
    in_band = (first_y < row_start + tile_rows) & (last_y >= row_start)
    hit = (
        jnp.broadcast_to(in_band, (groups, nets))
        & (first_x < group_at + group_cols)
        & (last_x >= group_at)
    )
    hit = jnp.where(hit, 1.0, 0.0)
    chunks = nets // LANES
    stacked = jnp.concatenate(
        [hit[:, k * LANES : (k + 1) * LANES] for k in range(chunks)], axis=0
    ).astype(BF16)
    below = (iota((LANES, LANES), 0) < iota((LANES, LANES), 1)).astype(F32).astype(BF16)
    before = contract(stacked, below, 1, 0)
    whole = contract(stacked, jnp.ones((LANES, LANES), BF16), 1, 0)
    offset = jnp.zeros((groups, LANES), F32)
    ranks = []
    for k in range(chunks):
        rows = slice(k * groups, (k + 1) * groups)
        ranks.append(before[rows] + offset)
        offset = offset + whole[rows]
    rank = jnp.concatenate(ranks, axis=1)
    rank = jnp.clip(rank - base.astype(F32), -1.0, float(SLOTS))
    rank = jnp.where(hit > 0.0, rank, -1.0)
    largest = jnp.max(offset, axis=0, keepdims=True)

    slot = iota((SLOTS, nets), 0).astype(F32).astype(BF16)
    field = iota((8, SLOTS), 0)
    for group in range(groups):
        mine = jnp.broadcast_to(rank[group : group + 1, :], (16, nets)).astype(BF16)
        mine = jnp.concatenate([mine] * (SLOTS // 16), axis=0)
        chosen = jnp.where(slot == mine, BF16(1), BF16(0))
        got = contract(vals, chosen, 1, 1)
        row = got[0:8] * 256.0 + got[8:16]
        row = jnp.where(field == 5, jnp.broadcast_to(largest, (8, SLOTS)), row)
        for at, peer in enumerate(order):
            if peer * groups // peers == group:
                out_ref[at] = row


def cells_kernel(tile_rows, tile_cols, bins_ref, area_ref, below_ref, sums_ref):
    cells = bins_ref.shape[1]
    bin_row = lax.shift_right_logical(bins_ref[...], 7)
    bin_col = bins_ref[...] & 127
    area = area_ref[...]
    reach = jnp.where(iota((tile_rows, cells), 0) <= bin_row, 1.0, 0.0).astype(BF16)
    is_col = iota((tile_cols, cells), 0) == bin_col
    pieces = jnp.concatenate(
        [jnp.where(is_col, part.astype(F32), 0.0).astype(BF16) for part in three_parts(area)],
        axis=0,
    )
    below = contract(reach, pieces, 1, 1)
    below = (
        below[:, :tile_cols] + below[:, tile_cols : 2 * tile_cols] + below[:, 2 * tile_cols :]
    )
    below_ref[...] = below
    area_sum = lane_sums(area)
    at = iota((8, LANES), 0)
    sums_ref[...] = jnp.where(
        at == 0,
        jnp.broadcast_to(below[0:1], (8, LANES)),
        jnp.broadcast_to(area_sum, (8, LANES)),
    )


def lane_sums(row):
    total = row[:, :LANES]
    for k in range(1, row.shape[1] // LANES):
        total = total + row[:, k * LANES : (k + 1) * LANES]
    return total


def tall(row, rows):
    short = jnp.broadcast_to(row, (16, row.shape[1])).astype(BF16)
    return jnp.concatenate([short] * (rows // 16), axis=0)


def inside(first, last, start, count):
    first = jnp.clip(first - start, 0.0, float(count))
    last = jnp.clip(last - start, -1.0, float(count - 1))
    return tall(first, count), tall(last, count)


def tile_kernel(
    has_past,
    nets_ref,
    capacity_ref,
    below_ref,
    sums_ref,
    *refs,
):
    if has_past:
        past_ref, *refs = refs
    rudy_ref, pay_ref = refs
    tile_rows, tile_cols = capacity_ref.shape
    row_start = lax.axis_index(ROW) * tile_rows
    col_start = lax.axis_index(COL) * tile_cols
    peers = nets_ref.shape[0]
    half = 256
    at = iota((half, SLOTS), 0).astype(F32).astype(BF16)
    col_at = at[:tile_cols]
    largest = jnp.zeros((1, SLOTS), F32)
    starts = [col_start.astype(F32)] + [
        (row_start + first).astype(F32) for first in range(0, tile_rows, half)
    ]
    rudy = jnp.zeros((tile_rows, tile_cols), F32)
    step = 4
    for peer in range(0, peers, step):
        hits, cols = [], []
        for box in [nets_ref[peer + k] for k in range(step)]:
            largest = jnp.maximum(largest, box[5:6])
            hit = []
            for first in starts[1:]:
                low, high = inside(box[2:3], box[3:4], first, half)
                hit.append(
                    jnp.where((at >= low) & (at <= high), BF16(1), BF16(0))
                )
            hits.append(jnp.concatenate(hit, axis=0))
            low, high = inside(box[0:1], box[1:2], starts[0], tile_cols)
            weight = tall(box[4:5], tile_cols)
            cols.append(jnp.where((col_at >= low) & (col_at <= high), weight, BF16(0)))
        rudy = rudy + contract(
            jnp.concatenate(hits, axis=1), jnp.concatenate(cols, axis=1), 1, 1
        )
    if has_past:
        rudy = rudy + past_ref[...]
    rudy_ref[...] = rudy
    excess = jnp.maximum(rudy - capacity_ref[...], 0.0)
    col_sum = jnp.sum(excess, axis=0, keepdims=True)
    weighed = jnp.sum(excess * below_ref[...], axis=0, keepdims=True)
    at = iota((8, LANES), 0) & 3
    shared = halves(sums_ref[1:2], weighed)
    pay = jnp.broadcast_to(largest, (8, LANES))
    for k, row in enumerate((col_sum, sums_ref[0:1], shared)):
        pay = jnp.where(at == k, jnp.broadcast_to(row, (8, LANES)), pay)
    for k in range(pay_ref.shape[0] // 8):
        pay_ref[8 * k : 8 * k + 8] = pay


def halves(a, b):
    half = LANES // 2
    lower = iota((1, LANES), 1) < half
    return jnp.where(lower, a + pltpu.roll(a, half, 1), b + pltpu.roll(b, half, 1))


def inflation_kernel(
    factor, rudy_ref, capacity_ref, bins_ref, carried_ref, inflation_ref, looked_ref
):
    tile_rows, tile_cols = rudy_ref.shape
    excess = jnp.maximum(rudy_ref[...] - capacity_ref[...], 0.0)
    half = 256
    lower = (iota((half, half), 0) >= iota((half, half), 1)).astype(F32).astype(BF16)
    carry = jnp.zeros((1, tile_cols), F32)
    parts = []
    for start in range(0, tile_rows, half):
        pieces = jnp.concatenate(three_parts(excess[start : start + half]), axis=1)
        sums = contract(lower, pieces, 1, 0)
        part = (
            sums[:, :tile_cols]
            + sums[:, tile_cols : 2 * tile_cols]
            + sums[:, 2 * tile_cols :]
            + carry
        )
        parts.append(part)
        carry = part[half - 1 : half, :]
    within = jnp.concatenate(parts, axis=0)
    inflation_ref[...] = 1.0 + factor * (within + carried_ref[0:1])

    cells = bins_ref.shape[1]
    bin_row = lax.shift_right_logical(bins_ref[...], 7)
    bin_col = bins_ref[...] & 127
    row_hot = jnp.where(iota((tile_rows, cells), 0) == bin_row, 1.0, 0.0).astype(BF16)
    turned = jnp.concatenate(three_parts(within.T), axis=0)
    picked = contract(turned, row_hot, 1, 0)
    picked = (
        picked[:tile_cols] + picked[tile_cols : 2 * tile_cols] + picked[2 * tile_cols :]
    )
    is_col = iota((tile_cols, cells), 0) == bin_col
    looked_ref[...] = jnp.sum(jnp.where(is_col, picked, 0.0), axis=0, keepdims=True)


def carry_kernel(order, rows, pays_ref, *refs):
    *base_ref, carried_ref, totals_ref, base_out, left_ref = refs
    base = (base_ref[0][0] if base_ref else 0) + SLOTS
    row_me = lax.axis_index(ROW)
    col_me = lax.axis_index(("col_1", "col_2"))
    width = pays_ref.shape[0] // (4 * rows)
    mine = jnp.zeros((1, LANES), F32)
    bilinear = jnp.zeros((1, LANES), F32)
    shared = jnp.zeros((1, LANES), F32)
    largest = jnp.zeros((1, LANES), F32)
    for col in range(width):
        running = jnp.zeros((1, LANES), F32)
        for row in range(rows):
            at = 4 * order.index(row * width + col)
            pay = pays_ref[at : at + 4]
            mine = jnp.where((row_me == row) & (col_me == col), running, mine)
            bilinear = bilinear + pay[1:2] * running
            shared = shared + pay[2:3]
            largest = jnp.maximum(largest, pay[3:4])
            running = running + pay[0:1]
    base_out[0] = jnp.int32(base)
    left_ref[0] = jnp.max(largest).astype(jnp.int32) - base
    carried_ref[...] = jnp.broadcast_to(mine, carried_ref.shape)
    totals = shared + halves(jnp.zeros((1, LANES), F32), bilinear)
    totals_ref[...] = jnp.broadcast_to(totals, totals_ref.shape)


def sizes_kernel(factor, carried_ref, totals_ref, bins_ref, area_ref, looked_ref, sizes_ref):
    totals = jnp.sum(totals_ref[...], axis=0, keepdims=True)
    lower = iota(totals.shape, 1) < LANES // 2
    area_total = jnp.sum(jnp.where(lower, totals, 0.0), axis=1, keepdims=True)
    added = jnp.sum(jnp.where(lower, 0.0, totals), axis=1, keepdims=True)
    grown_total = area_total + factor * added
    bin_col = bins_ref[...] & 127
    above = jnp.take_along_axis(
        jnp.broadcast_to(carried_ref[0:1], bin_col.shape), bin_col, axis=1
    )
    grown = area_ref[...] * (1.0 + factor * (looked_ref[...] + above))
    sizes_ref[...] = grown * (area_total / grown_total)


def call(kernel, outs, args, scratch=(), limit=16, flops=1_000_000):
    smem = pl.BlockSpec(memory_space=pltpu.SMEM)
    vmem = pl.BlockSpec(memory_space=pltpu.VMEM)
    outs = [o if isinstance(o, jax.ShapeDtypeStruct) else jax.ShapeDtypeStruct(o, F32) for o in outs]
    return pl.pallas_call(
        kernel,
        out_shape=outs,
        in_specs=[smem if a.ndim == 1 else vmem for a in args],
        out_specs=[smem if len(o.shape) == 1 else vmem for o in outs],
        scratch_shapes=list(scratch),
        compiler_params=pltpu.CompilerParams(vmem_limit_bytes=limit * 1024 * 1024),
        cost_estimate=pl.CostEstimate(flops=flops, bytes_accessed=1_000_000, transcendentals=0),
    )(*args)


def hops(a, b, size):
    return min((a - b) % size, (b - a) % size)


def peer_order(names):
    sizes = [lax.axis_size(name) for name in names]
    full = {name: lax.axis_size(name) for name in ROW + COL}
    y_size = full["row_1"] * full["col_1"]
    places = []
    for index in range(math.prod(sizes)):
        at, rest = {}, index
        for name, size in reversed(list(zip(names, sizes))):
            at[name] = rest % size
            rest //= size
        away = 0.0
        for name in ("row_0", "col_0"):
            if name in at:
                away += hops(at[name], full[name] // 2, full[name])
        if "row_1" in at:
            away += hops(at["row_1"] * full["col_1"] + at["col_1"], y_size // 2, y_size)
        elif "col_1" in at:
            away += full["col_1"] - 1 - at["col_1"]
        if "col_2" in at:
            away += 0.5 * (full["col_2"] - 1 - at["col_2"])
        places.append((-away, index))
    root = max(places)
    return [root[1]] + [p[1] for p in sorted(places) if p != root]


def exchange(payload, axis, order):
    return lax.all_to_all(payload, axis, 0, 0, axis_index_groups=[order], tiled=True)


def per_device(boxes, pins, capacity, cell_bin, cell_area):
    tile_rows, tile_cols = capacity.shape
    rows, cols = lax.axis_size(ROW), lax.axis_size(COL)
    groups = lax.axis_size("col_0")
    nets = boxes.shape[1]
    cells = cell_bin.shape[1]
    factor = 2.0 / (tile_rows * rows)
    near = lax.axis_size(NEAR)
    col_order = peer_order(COL)
    near_order = peer_order(NEAR)
    far_order = peer_order(("col_0",))
    pins = pins.reshape(1, nets)
    below, cell_sums = call(
        functools.partial(cells_kernel, tile_rows, tile_cols),
        [(tile_rows, tile_cols), (8, LANES)],
        (cell_bin, cell_area),
        flops=4_000_000_000,
    )

    def one_round(base, past):
        (packed,) = call(
            functools.partial(
                pack_kernel, col_order, cols, groups, tile_cols * (cols // groups), tile_rows
            ),
            [(cols, 8, SLOTS)],
            (boxes, pins) + base,
            [pltpu.VMEM((16, nets), F32)],
        )
        mine = exchange(packed, COL, col_order)
        rudy, pay = call(
            functools.partial(tile_kernel, past is not None),
            [(tile_rows, tile_cols), (near * 4, LANES)],
            (mine, capacity, below, cell_sums)
            + (() if past is None else (past,)),
            limit=28,
        )
        pays = exchange(pay.reshape(near, 4, LANES), NEAR, near_order).reshape(near * 4, LANES)
        one = jax.ShapeDtypeStruct((1,), jnp.int32)
        carried, totals, reached, left = call(
            functools.partial(carry_kernel, near_order, rows),
            [(8, LANES), (groups, LANES), one, one],
            (pays,) + base,
        )
        return left, reached, rudy, carried, totals

    def unfinished(state):
        return state[0][0] > 0

    def next_round(state):
        return one_round((state[1],), state[2])

    first = one_round((), None)
    _, _, rudy, carried, totals = lax.cond(
        unfinished(first),
        lambda state: lax.while_loop(unfinished, next_round, state),
        lambda state: state,
        first,
    )

    totals = exchange(totals, "col_0", far_order)
    shape = (cells // LANES, LANES)
    inflation, looked = call(
        functools.partial(inflation_kernel, factor),
        [(tile_rows, tile_cols), (1, cells)],
        (rudy, capacity, cell_bin, carried),
        limit=28,
        flops=4_000_000_000,
    )
    (sizes,) = call(
        functools.partial(sizes_kernel, factor),
        [shape],
        (carried, totals, cell_bin.reshape(shape), cell_area.reshape(shape), looked.reshape(shape)),
    )
    return rudy, inflation, sizes.reshape(cell_area.shape)


def solution(mesh):
    split = Mesh(mesh.devices.reshape(4, 2, 8, 2, 2), ROW + COL)
    placed = (P(None, COL), P(COL), P(ROW, COL), P(ROW, COL), P(ROW, COL))
    return jax.shard_map(
        per_device,
        mesh=split,
        in_specs=placed,
        out_specs=(P(ROW, COL), P(ROW, COL), P(ROW, COL)),
        check_vma=False,
    )
```

```python
import functools
import math

import jax
import jax.numpy as jnp
from jax import lax
from jax.experimental import pallas as pl
from jax.experimental.pallas import tpu as pltpu
from jax.sharding import Mesh
from jax.sharding import PartitionSpec as P

ROW = ("row_0", "row_1")
COL = ("col_0", "col_1", "col_2")
NEAR = ("row_0", "row_1", "col_1", "col_2")
SLOTS = 128
LANES = 128
F32 = jnp.float32
BF16 = jnp.bfloat16


def iota(shape, dim):
    return lax.broadcasted_iota(jnp.int32, shape, dim)


def contract(a, b, dim_a, dim_b):
    return lax.dot_general(
        a, b, (((dim_a,), (dim_b,)), ((), ())), preferred_element_type=F32
    )


def three_parts(x):
    high = x.astype(BF16)
    rest = x - high.astype(F32)
    middle = rest.astype(BF16)
    low = (rest - middle.astype(F32)).astype(BF16)
    return high, middle, low


def two_parts(x):
    high = x.astype(BF16)
    return high, (x - high.astype(F32)).astype(BF16)


def pack_kernel(
    order, peers, groups, group_cols, tile_rows, boxes_ref, pins_ref, *refs
):
    nets = boxes_ref.shape[1]
    *base_ref, out_ref, vals_ref = refs
    base = base_ref[0][0] if base_ref else jnp.int32(0)
    row_start = lax.axis_index(ROW) * tile_rows
    first_x, last_x = boxes_ref[0:1, :], boxes_ref[1:2, :]
    first_y, last_y = boxes_ref[2:3, :], boxes_ref[3:4, :]
    span_x = (last_x - first_x + 1).astype(F32)
    span_y = (last_y - first_y + 1).astype(F32)
    weight = jnp.log(pins_ref[...].astype(F32)) * (span_x + span_y) / (span_x * span_y)
    weight = weight.astype(BF16).astype(F32)
    vals_ref[...] = jnp.zeros_like(vals_ref)
    vals_ref[0:4, :] = lax.shift_right_logical(boxes_ref[...], 8).astype(F32)
    vals_ref[4:5, :] = weight * (1.0 / 256.0)
    vals_ref[8:12, :] = (boxes_ref[...] & 255).astype(F32)
    vals = vals_ref[...].astype(BF16)

    group_at = iota((groups, nets), 0) * group_cols
    in_band = (first_y < row_start + tile_rows) & (last_y >= row_start)
    hit = (
        jnp.broadcast_to(in_band, (groups, nets))
        & (first_x < group_at + group_cols)
        & (last_x >= group_at)
    )
    hit = jnp.where(hit, 1.0, 0.0)
    chunks = nets // LANES
    stacked = jnp.concatenate(
        [hit[:, k * LANES : (k + 1) * LANES] for k in range(chunks)], axis=0
    ).astype(BF16)
    below = (iota((LANES, LANES), 0) < iota((LANES, LANES), 1)).astype(F32).astype(BF16)
    before = contract(stacked, below, 1, 0)
    whole = contract(stacked, jnp.ones((LANES, LANES), BF16), 1, 0)
    offset = jnp.zeros((groups, LANES), F32)
    ranks = []
    for k in range(chunks):
        rows = slice(k * groups, (k + 1) * groups)
        ranks.append(before[rows] + offset)
        offset = offset + whole[rows]
    rank = jnp.concatenate(ranks, axis=1)
    rank = jnp.clip(rank - base.astype(F32), -1.0, float(SLOTS))
    rank = jnp.where(hit > 0.0, rank, -1.0)
    largest = jnp.max(offset, axis=0, keepdims=True)

    slot = iota((SLOTS, nets), 0).astype(F32).astype(BF16)
    field = iota((8, SLOTS), 0)
    for group in range(groups):
        mine = jnp.broadcast_to(rank[group : group + 1, :], (16, nets)).astype(BF16)
        mine = jnp.concatenate([mine] * (SLOTS // 16), axis=0)
        chosen = jnp.where(slot == mine, BF16(1), BF16(0))
        got = contract(vals, chosen, 1, 1)
        row = got[0:8] * 256.0 + got[8:16]
        row = jnp.where(field == 5, jnp.broadcast_to(largest, (8, SLOTS)), row)
        for at, peer in enumerate(order):
            if peer * groups // peers == group:
                out_ref[at] = row


def cells_kernel(tile_rows, tile_cols, bins_ref, area_ref, below_ref, sums_ref):
    cells = bins_ref.shape[1]
    bin_row = lax.shift_right_logical(bins_ref[...], 7)
    bin_col = bins_ref[...] & 127
    area = area_ref[...]
    reach = jnp.where(iota((tile_rows, cells), 0) <= bin_row, 1.0, 0.0).astype(BF16)
    is_col = iota((tile_cols, cells), 0) == bin_col
    pieces = jnp.concatenate(
        [jnp.where(is_col, part.astype(F32), 0.0).astype(BF16) for part in three_parts(area)],
        axis=0,
    )
    below = contract(reach, pieces, 1, 1)
    below = (
        below[:, :tile_cols] + below[:, tile_cols : 2 * tile_cols] + below[:, 2 * tile_cols :]
    )
    below_ref[...] = below
    area_sum = lane_sums(area)
    at = iota((8, LANES), 0)
    sums_ref[...] = jnp.where(
        at == 0,
        jnp.broadcast_to(below[0:1], (8, LANES)),
        jnp.broadcast_to(area_sum, (8, LANES)),
    )


def lane_sums(row):
    total = row[:, :LANES]
    for k in range(1, row.shape[1] // LANES):
        total = total + row[:, k * LANES : (k + 1) * LANES]
    return total


def tall(row, rows):
    short = jnp.broadcast_to(row, (16, row.shape[1])).astype(BF16)
    return jnp.concatenate([short] * (rows // 16), axis=0)


def inside(first, last, start, count):
    first = jnp.clip(first - start, 0.0, float(count))
    last = jnp.clip(last - start, -1.0, float(count - 1))
    return tall(first, count), tall(last, count)


def tile_kernel(
    has_past,
    nets_ref,
    capacity_ref,
    below_ref,
    sums_ref,
    *refs,
):
    if has_past:
        past_ref, *refs = refs
    rudy_ref, pay_ref = refs
    tile_rows, tile_cols = capacity_ref.shape
    row_start = lax.axis_index(ROW) * tile_rows
    col_start = lax.axis_index(COL) * tile_cols
    peers = nets_ref.shape[0]
    half = 256
    at = iota((half, SLOTS), 0).astype(F32).astype(BF16)
    col_at = at[:tile_cols]
    largest = jnp.zeros((1, SLOTS), F32)
    starts = [col_start.astype(F32)] + [
        (row_start + first).astype(F32) for first in range(0, tile_rows, half)
    ]
    rudy = jnp.zeros((tile_rows, tile_cols), F32)
    step = 4
    for peer in range(0, peers, step):
        hits, cols = [], []
        for box in [nets_ref[peer + k] for k in range(step)]:
            largest = jnp.maximum(largest, box[5:6])
            hit = []
            for first in starts[1:]:
                low, high = inside(box[2:3], box[3:4], first, half)
                hit.append(
                    jnp.where((at >= low) & (at <= high), BF16(1), BF16(0))
                )
            hits.append(jnp.concatenate(hit, axis=0))
            low, high = inside(box[0:1], box[1:2], starts[0], tile_cols)
            weight = tall(box[4:5], tile_cols)
            cols.append(jnp.where((col_at >= low) & (col_at <= high), weight, BF16(0)))
        rudy = rudy + contract(
            jnp.concatenate(hits, axis=1), jnp.concatenate(cols, axis=1), 1, 1
        )
    if has_past:
        rudy = rudy + past_ref[...]
    rudy_ref[...] = rudy
    excess = jnp.maximum(rudy - capacity_ref[...], 0.0)
    col_sum = jnp.sum(excess, axis=0, keepdims=True)
    weighed = jnp.sum(excess * below_ref[...], axis=0, keepdims=True)
    at = iota((8, LANES), 0) & 3
    shared = halves(sums_ref[1:2], weighed)
    pay = jnp.broadcast_to(largest, (8, LANES))
    for k, row in enumerate((col_sum, sums_ref[0:1], shared)):
        pay = jnp.where(at == k, jnp.broadcast_to(row, (8, LANES)), pay)
    for k in range(pay_ref.shape[0] // 8):
        pay_ref[8 * k : 8 * k + 8] = pay


def halves(a, b):
    half = LANES // 2
    lower = iota((1, LANES), 1) < half
    return jnp.where(lower, a + pltpu.roll(a, half, 1), b + pltpu.roll(b, half, 1))


def near_row(row, count):
    return tall(jnp.clip(row.astype(F32), -1.0, float(count)), count)


def inflation_kernel(
    factor, rudy_ref, capacity_ref, bins_ref, carried_ref, inflation_ref, looked_ref
):
    tile_rows, tile_cols = rudy_ref.shape
    excess = jnp.maximum(rudy_ref[...] - capacity_ref[...], 0.0)
    half = 256
    lower = (iota((half, half), 0) >= iota((half, half), 1)).astype(F32).astype(BF16)
    carry = jnp.zeros((1, tile_cols), F32)
    parts = []
    for start in range(0, tile_rows, half):
        pieces = jnp.concatenate(two_parts(excess[start : start + half]), axis=1)
        sums = contract(lower, pieces, 1, 0)
        part = sums[:, :tile_cols] + sums[:, tile_cols:] + carry
        parts.append(part)
        carry = part[half - 1 : half, :]
    within = jnp.concatenate(parts, axis=0)
    inflation_ref[...] = 1.0 + factor * (within + carried_ref[0:1])

    cells = bins_ref.shape[1]
    bin_row = lax.shift_right_logical(bins_ref[...], 7)
    bin_col = bins_ref[...] & 127
    at = iota((half, cells), 0).astype(F32).astype(BF16)
    row_hot = jnp.concatenate(
        [
            jnp.where(at == near_row(bin_row - start, half), BF16(1), BF16(0))
            for start in range(0, tile_rows, half)
        ],
        axis=0,
    )
    turned = jnp.concatenate(two_parts(within.T), axis=0)
    picked = contract(turned, row_hot, 1, 0)
    picked = picked[:tile_cols] + picked[tile_cols:]
    is_col = iota((tile_cols, cells), 0) == bin_col
    looked_ref[...] = jnp.sum(jnp.where(is_col, picked, 0.0), axis=0, keepdims=True)


def carry_kernel(order, rows, pays_ref, *refs):
    *base_ref, carried_ref, totals_ref, base_out, left_ref = refs
    base = (base_ref[0][0] if base_ref else 0) + SLOTS
    row_me = lax.axis_index(ROW)
    col_me = lax.axis_index(("col_1", "col_2"))
    width = pays_ref.shape[0] // (4 * rows)
    mine = jnp.zeros((1, LANES), F32)
    bilinear = jnp.zeros((1, LANES), F32)
    shared = jnp.zeros((1, LANES), F32)
    largest = jnp.zeros((1, LANES), F32)
    for col in range(width):
        running = jnp.zeros((1, LANES), F32)
        for row in range(rows):
            at = 4 * order.index(row * width + col)
            pay = pays_ref[at : at + 4]
            mine = jnp.where((row_me == row) & (col_me == col), running, mine)
            bilinear = bilinear + pay[1:2] * running
            shared = shared + pay[2:3]
            largest = jnp.maximum(largest, pay[3:4])
            running = running + pay[0:1]
    base_out[0] = jnp.int32(base)
    left_ref[0] = jnp.max(largest).astype(jnp.int32) - base
    carried_ref[...] = jnp.broadcast_to(mine, carried_ref.shape)
    totals = shared + halves(jnp.zeros((1, LANES), F32), bilinear)
    totals_ref[...] = jnp.broadcast_to(totals, totals_ref.shape)


def sizes_kernel(factor, carried_ref, totals_ref, bins_ref, area_ref, looked_ref, sizes_ref):
    totals = jnp.sum(totals_ref[...], axis=0, keepdims=True)
    lower = iota(totals.shape, 1) < LANES // 2
    area_total = jnp.sum(jnp.where(lower, totals, 0.0), axis=1, keepdims=True)
    added = jnp.sum(jnp.where(lower, 0.0, totals), axis=1, keepdims=True)
    grown_total = area_total + factor * added
    bin_col = bins_ref[...] & 127
    above = jnp.take_along_axis(
        jnp.broadcast_to(carried_ref[0:1], bin_col.shape), bin_col, axis=1
    )
    grown = area_ref[...] * (1.0 + factor * (looked_ref[...] + above))
    sizes_ref[...] = grown * (area_total / grown_total)


def call(kernel, outs, args, scratch=(), limit=16, flops=1_000_000):
    smem = pl.BlockSpec(memory_space=pltpu.SMEM)
    vmem = pl.BlockSpec(memory_space=pltpu.VMEM)
    outs = [o if isinstance(o, jax.ShapeDtypeStruct) else jax.ShapeDtypeStruct(o, F32) for o in outs]
    return pl.pallas_call(
        kernel,
        out_shape=outs,
        in_specs=[smem if a.ndim == 1 else vmem for a in args],
        out_specs=[smem if len(o.shape) == 1 else vmem for o in outs],
        scratch_shapes=list(scratch),
        compiler_params=pltpu.CompilerParams(vmem_limit_bytes=limit * 1024 * 1024),
        cost_estimate=pl.CostEstimate(flops=flops, bytes_accessed=1_000_000, transcendentals=0),
    )(*args)


def hops(a, b, size):
    return min((a - b) % size, (b - a) % size)


def peer_order(names):
    sizes = [lax.axis_size(name) for name in names]
    full = {name: lax.axis_size(name) for name in ROW + COL}
    y_size = full["row_1"] * full["col_1"]
    middle = full["col_0"] // 2 + (names == COL)
    places = []
    for index in range(math.prod(sizes)):
        at, rest = {}, index
        for name, size in reversed(list(zip(names, sizes))):
            at[name] = rest % size
            rest //= size
        away = 0.0
        if "row_0" in at:
            away += hops(at["row_0"], full["row_0"] // 2, full["row_0"])
        if "col_0" in at:
            away += hops(at["col_0"], middle, full["col_0"])
        if "row_1" in at:
            away += hops(at["row_1"] * full["col_1"] + at["col_1"], y_size // 2, y_size)
        elif "col_1" in at:
            away += at["col_1"]
        if "col_2" in at:
            away += 0.5 * (full["col_2"] - 1 - at["col_2"])
        places.append((-away, index))
    root = max(places)
    return [root[1]] + [p[1] for p in sorted(places) if p != root]


def exchange(payload, axis, order):
    return lax.all_to_all(payload, axis, 0, 0, axis_index_groups=[order], tiled=True)


def per_device(boxes, pins, capacity, cell_bin, cell_area):
    tile_rows, tile_cols = capacity.shape
    rows, cols = lax.axis_size(ROW), lax.axis_size(COL)
    groups = lax.axis_size("col_0")
    nets = boxes.shape[1]
    cells = cell_bin.shape[1]
    factor = 2.0 / (tile_rows * rows)
    near = lax.axis_size(NEAR)
    col_order = peer_order(COL)
    near_order = peer_order(NEAR)
    far_order = peer_order(("col_0",))
    pins = pins.reshape(1, nets)
    below, cell_sums = call(
        functools.partial(cells_kernel, tile_rows, tile_cols),
        [(tile_rows, tile_cols), (8, LANES)],
        (cell_bin, cell_area),
        flops=4_000_000_000,
    )

    def one_round(base, past):
        (packed,) = call(
            functools.partial(
                pack_kernel, col_order, cols, groups, tile_cols * (cols // groups), tile_rows
            ),
            [(cols, 8, SLOTS)],
            (boxes, pins) + base,
            [pltpu.VMEM((16, nets), F32)],
        )
        mine = exchange(packed, COL, col_order)
        rudy, pay = call(
            functools.partial(tile_kernel, past is not None),
            [(tile_rows, tile_cols), (near * 4, LANES)],
            (mine, capacity, below, cell_sums)
            + (() if past is None else (past,)),
            limit=28,
        )
        pays = exchange(pay.reshape(near, 4, LANES), NEAR, near_order).reshape(near * 4, LANES)
        one = jax.ShapeDtypeStruct((1,), jnp.int32)
        carried, totals, reached, left = call(
            functools.partial(carry_kernel, near_order, rows),
            [(8, LANES), (groups, LANES), one, one],
            (pays,) + base,
        )
        return left, reached, rudy, carried, totals

    def unfinished(state):
        return state[0][0] > 0

    def next_round(state):
        return one_round((state[1],), state[2])

    first = one_round((), None)
    _, _, rudy, carried, totals = lax.cond(
        unfinished(first),
        lambda state: lax.while_loop(unfinished, next_round, state),
        lambda state: state,
        first,
    )

    totals = exchange(totals, "col_0", far_order)
    shape = (cells // LANES, LANES)
    inflation, looked = call(
        functools.partial(inflation_kernel, factor),
        [(tile_rows, tile_cols), (1, cells)],
        (rudy, capacity, cell_bin, carried),
        limit=28,
        flops=4_000_000_000,
    )
    (sizes,) = call(
        functools.partial(sizes_kernel, factor),
        [shape],
        (carried, totals, cell_bin.reshape(shape), cell_area.reshape(shape), looked.reshape(shape)),
    )
    return rudy, inflation, sizes.reshape(cell_area.shape)


def solution(mesh):
    split = Mesh(mesh.devices.reshape(4, 2, 8, 2, 2), ROW + COL)
    placed = (P(None, COL), P(COL), P(ROW, COL), P(ROW, COL), P(ROW, COL))
    return jax.shard_map(
        per_device,
        mesh=split,
        in_specs=placed,
        out_specs=(P(ROW, COL), P(ROW, COL), P(ROW, COL)),
        check_vma=False,
    )
```

```python
import functools
import math

import jax
import jax.numpy as jnp
from jax import lax
from jax.experimental import pallas as pl
from jax.experimental.pallas import tpu as pltpu
from jax.sharding import Mesh
from jax.sharding import PartitionSpec as P

ROW = ("row_0", "row_1")
COL = ("col_0", "col_1", "col_2")
NEAR = ("row_0", "row_1", "col_1", "col_2")
SLOTS = 128
LANES = 128
F32 = jnp.float32
BF16 = jnp.bfloat16


def iota(shape, dim):
    return lax.broadcasted_iota(jnp.int32, shape, dim)


def contract(a, b, dim_a, dim_b):
    return lax.dot_general(
        a, b, (((dim_a,), (dim_b,)), ((), ())), preferred_element_type=F32
    )


def three_parts(x):
    high = x.astype(BF16)
    rest = x - high.astype(F32)
    middle = rest.astype(BF16)
    low = (rest - middle.astype(F32)).astype(BF16)
    return high, middle, low


def two_parts(x):
    high = x.astype(BF16)
    return high, (x - high.astype(F32)).astype(BF16)


def pack_kernel(
    order, peers, groups, group_cols, tile_rows, boxes_ref, pins_ref, *refs
):
    nets = boxes_ref.shape[1]
    *base_ref, out_ref, vals_ref = refs
    base = base_ref[0][0] if base_ref else jnp.int32(0)
    row_start = lax.axis_index(ROW) * tile_rows
    first_x, last_x = boxes_ref[0:1, :], boxes_ref[1:2, :]
    first_y, last_y = boxes_ref[2:3, :], boxes_ref[3:4, :]
    span_x = (last_x - first_x + 1).astype(F32)
    span_y = (last_y - first_y + 1).astype(F32)
    weight = jnp.log(pins_ref[...].astype(F32)) * (span_x + span_y) / (span_x * span_y)
    weight = weight.astype(BF16).astype(F32)
    vals_ref[...] = jnp.zeros_like(vals_ref)
    vals_ref[0:4, :] = lax.shift_right_logical(boxes_ref[...], 8).astype(F32)
    vals_ref[4:5, :] = weight * (1.0 / 256.0)
    vals_ref[8:12, :] = (boxes_ref[...] & 255).astype(F32)
    vals = vals_ref[...].astype(BF16)

    group_at = iota((groups, nets), 0) * group_cols
    in_band = (first_y < row_start + tile_rows) & (last_y >= row_start)
    hit = (
        jnp.broadcast_to(in_band, (groups, nets))
        & (first_x < group_at + group_cols)
        & (last_x >= group_at)
    )
    hit = jnp.where(hit, 1.0, 0.0)
    chunks = nets // LANES
    stacked = jnp.concatenate(
        [hit[:, k * LANES : (k + 1) * LANES] for k in range(chunks)], axis=0
    ).astype(BF16)
    below = (iota((LANES, LANES), 0) < iota((LANES, LANES), 1)).astype(F32).astype(BF16)
    before = contract(stacked, below, 1, 0)
    whole = contract(stacked, jnp.ones((LANES, LANES), BF16), 1, 0)
    offset = jnp.zeros((groups, LANES), F32)
    ranks = []
    for k in range(chunks):
        rows = slice(k * groups, (k + 1) * groups)
        ranks.append(before[rows] + offset)
        offset = offset + whole[rows]
    rank = jnp.concatenate(ranks, axis=1)
    rank = jnp.clip(rank - base.astype(F32), -1.0, float(SLOTS))
    rank = jnp.where(hit > 0.0, rank, -1.0)
    largest = jnp.max(offset, axis=0, keepdims=True)

    slot = iota((SLOTS, nets), 0).astype(F32).astype(BF16)
    field = iota((8, SLOTS), 0)
    for pair in range(0, groups, 2):
        chosen = []
        for group in (pair, pair + 1):
            mine = jnp.broadcast_to(rank[group : group + 1, :], (16, nets)).astype(BF16)
            mine = jnp.concatenate([mine] * (SLOTS // 16), axis=0)
            chosen.append(jnp.where(slot == mine, BF16(1), BF16(0)))
        both = contract(vals, jnp.concatenate(chosen, axis=0), 1, 1)
        for group in (pair, pair + 1):
            got = both[:, (group - pair) * SLOTS : (group - pair + 1) * SLOTS]
            row = got[0:8] * 256.0 + got[8:16]
            row = jnp.where(field == 5, jnp.broadcast_to(largest, (8, SLOTS)), row)
            for at, peer in enumerate(order):
                if peer * groups // peers == group:
                    out_ref[at] = row


def cells_kernel(tile_rows, tile_cols, bins_ref, area_ref, below_ref, sums_ref):
    cells = bins_ref.shape[1]
    bin_row = lax.shift_right_logical(bins_ref[...], 7)
    bin_col = bins_ref[...] & 127
    area = area_ref[...]
    reach = jnp.where(iota((tile_rows, cells), 0) <= bin_row, 1.0, 0.0).astype(BF16)
    is_col = iota((tile_cols, cells), 0) == bin_col
    pieces = jnp.concatenate(
        [jnp.where(is_col, part.astype(F32), 0.0).astype(BF16) for part in three_parts(area)],
        axis=0,
    )
    below = contract(reach, pieces, 1, 1)
    below = (
        below[:, :tile_cols] + below[:, tile_cols : 2 * tile_cols] + below[:, 2 * tile_cols :]
    )
    below_ref[...] = below
    area_sum = lane_sums(area)
    at = iota((8, LANES), 0)
    sums_ref[...] = jnp.where(
        at == 0,
        jnp.broadcast_to(below[0:1], (8, LANES)),
        jnp.broadcast_to(area_sum, (8, LANES)),
    )


def lane_sums(row):
    total = row[:, :LANES]
    for k in range(1, row.shape[1] // LANES):
        total = total + row[:, k * LANES : (k + 1) * LANES]
    return total


def tall(row, rows):
    short = jnp.broadcast_to(row, (16, row.shape[1])).astype(BF16)
    return jnp.concatenate([short] * (rows // 16), axis=0)


def inside(first, last, start, count):
    first = jnp.clip(first - start, 0.0, float(count))
    last = jnp.clip(last - start, -1.0, float(count - 1))
    return tall(first, count), tall(last, count)


def tile_kernel(
    has_past,
    nets_ref,
    capacity_ref,
    below_ref,
    sums_ref,
    *refs,
):
    if has_past:
        past_ref, *refs = refs
    rudy_ref, pay_ref = refs
    tile_rows, tile_cols = capacity_ref.shape
    row_start = lax.axis_index(ROW) * tile_rows
    col_start = lax.axis_index(COL) * tile_cols
    peers = nets_ref.shape[0]
    half = 256
    at = iota((half, SLOTS), 0).astype(F32).astype(BF16)
    col_at = at[:tile_cols]
    largest = jnp.zeros((1, SLOTS), F32)
    starts = [col_start.astype(F32)] + [
        (row_start + first).astype(F32) for first in range(0, tile_rows, half)
    ]
    rudy = jnp.zeros((tile_rows, tile_cols), F32)
    step = 8
    for peer in range(0, peers, step):
        hits, cols = [], []
        for box in [nets_ref[peer + k] for k in range(step)]:
            largest = jnp.maximum(largest, box[5:6])
            hit = []
            for first in starts[1:]:
                low, high = inside(box[2:3], box[3:4], first, half)
                hit.append(
                    jnp.where((at >= low) & (at <= high), BF16(1), BF16(0))
                )
            hits.append(jnp.concatenate(hit, axis=0))
            low, high = inside(box[0:1], box[1:2], starts[0], tile_cols)
            weight = tall(box[4:5], tile_cols)
            cols.append(jnp.where((col_at >= low) & (col_at <= high), weight, BF16(0)))
        rudy = rudy + contract(
            jnp.concatenate(hits, axis=1), jnp.concatenate(cols, axis=1), 1, 1
        )
    if has_past:
        rudy = rudy + past_ref[...]
    rudy_ref[...] = rudy
    excess = jnp.maximum(rudy - capacity_ref[...], 0.0)
    col_sum = jnp.sum(excess, axis=0, keepdims=True)
    weighed = jnp.sum(excess * below_ref[...], axis=0, keepdims=True)
    at = iota((8, LANES), 0) & 3
    shared = halves(sums_ref[1:2], weighed)
    pay = jnp.broadcast_to(largest, (8, LANES))
    for k, row in enumerate((col_sum, sums_ref[0:1], shared)):
        pay = jnp.where(at == k, jnp.broadcast_to(row, (8, LANES)), pay)
    for k in range(pay_ref.shape[0] // 8):
        pay_ref[8 * k : 8 * k + 8] = pay


def halves(a, b):
    half = LANES // 2
    lower = iota((1, LANES), 1) < half
    return jnp.where(lower, a + pltpu.roll(a, half, 1), b + pltpu.roll(b, half, 1))


def near_row(row, count):
    return tall(jnp.clip(row.astype(F32), -1.0, float(count)), count)


def inflation_kernel(
    factor, rudy_ref, capacity_ref, bins_ref, carried_ref, inflation_ref, looked_ref
):
    tile_rows, tile_cols = rudy_ref.shape
    excess = jnp.maximum(rudy_ref[...] - capacity_ref[...], 0.0)
    half = 256
    lower = (iota((half, half), 0) >= iota((half, half), 1)).astype(F32).astype(BF16)
    carry = jnp.zeros((1, tile_cols), F32)
    parts = []
    for start in range(0, tile_rows, half):
        pieces = jnp.concatenate(two_parts(excess[start : start + half]), axis=1)
        sums = contract(lower, pieces, 1, 0)
        part = sums[:, :tile_cols] + sums[:, tile_cols:] + carry
        parts.append(part)
        carry = part[half - 1 : half, :]
    within = jnp.concatenate(parts, axis=0)
    inflation_ref[...] = 1.0 + factor * (within + carried_ref[0:1])

    cells = bins_ref.shape[1]
    bin_row = lax.shift_right_logical(bins_ref[...], 7)
    bin_col = bins_ref[...] & 127
    at = iota((half, cells), 0).astype(F32).astype(BF16)
    row_hot = jnp.concatenate(
        [
            jnp.where(at == near_row(bin_row - start, half), BF16(1), BF16(0))
            for start in range(0, tile_rows, half)
        ],
        axis=0,
    )
    turned = jnp.concatenate(two_parts(within.T), axis=0)
    picked = contract(turned, row_hot, 1, 0)
    picked = picked[:tile_cols] + picked[tile_cols:]
    is_col = iota((tile_cols, cells), 0) == bin_col
    looked_ref[...] = jnp.sum(jnp.where(is_col, picked, 0.0), axis=0, keepdims=True)


def carry_kernel(order, rows, pays_ref, *refs):
    *base_ref, carried_ref, totals_ref, base_out, left_ref = refs
    base = (base_ref[0][0] if base_ref else 0) + SLOTS
    row_me = lax.axis_index(ROW)
    col_me = lax.axis_index(("col_1", "col_2"))
    width = pays_ref.shape[0] // (4 * rows)
    mine = jnp.zeros((1, LANES), F32)
    bilinear = jnp.zeros((1, LANES), F32)
    shared = jnp.zeros((1, LANES), F32)
    largest = jnp.zeros((1, LANES), F32)
    for col in range(width):
        running = jnp.zeros((1, LANES), F32)
        for row in range(rows):
            at = 4 * order.index(row * width + col)
            pay = pays_ref[at : at + 4]
            mine = jnp.where((row_me == row) & (col_me == col), running, mine)
            bilinear = bilinear + pay[1:2] * running
            shared = shared + pay[2:3]
            largest = jnp.maximum(largest, pay[3:4])
            running = running + pay[0:1]
    base_out[0] = jnp.int32(base)
    left_ref[0] = jnp.max(largest).astype(jnp.int32) - base
    carried_ref[...] = jnp.broadcast_to(mine, carried_ref.shape)
    totals = shared + halves(jnp.zeros((1, LANES), F32), bilinear)
    totals_ref[...] = jnp.broadcast_to(totals, totals_ref.shape)


def sizes_kernel(factor, carried_ref, totals_ref, bins_ref, area_ref, looked_ref, sizes_ref):
    totals = jnp.sum(totals_ref[...], axis=0, keepdims=True)
    lower = iota(totals.shape, 1) < LANES // 2
    area_total = jnp.sum(jnp.where(lower, totals, 0.0), axis=1, keepdims=True)
    added = jnp.sum(jnp.where(lower, 0.0, totals), axis=1, keepdims=True)
    grown_total = area_total + factor * added
    bin_col = bins_ref[...] & 127
    above = jnp.take_along_axis(
        jnp.broadcast_to(carried_ref[0:1], bin_col.shape), bin_col, axis=1
    )
    grown = area_ref[...] * (1.0 + factor * (looked_ref[...] + above))
    sizes_ref[...] = grown * (area_total / grown_total)


def call(kernel, outs, args, scratch=(), limit=16, flops=1_000_000):
    smem = pl.BlockSpec(memory_space=pltpu.SMEM)
    vmem = pl.BlockSpec(memory_space=pltpu.VMEM)
    outs = [o if isinstance(o, jax.ShapeDtypeStruct) else jax.ShapeDtypeStruct(o, F32) for o in outs]
    return pl.pallas_call(
        kernel,
        out_shape=outs,
        in_specs=[smem if a.ndim == 1 else vmem for a in args],
        out_specs=[smem if len(o.shape) == 1 else vmem for o in outs],
        scratch_shapes=list(scratch),
        compiler_params=pltpu.CompilerParams(vmem_limit_bytes=limit * 1024 * 1024),
        cost_estimate=pl.CostEstimate(flops=flops, bytes_accessed=1_000_000, transcendentals=0),
    )(*args)


def hops(a, b, size):
    return min((a - b) % size, (b - a) % size)


def peer_order(names):
    sizes = [lax.axis_size(name) for name in names]
    full = {name: lax.axis_size(name) for name in ROW + COL}
    y_size = full["row_1"] * full["col_1"]
    middle = full["col_0"] // 2 + (names == COL)
    places = []
    for index in range(math.prod(sizes)):
        at, rest = {}, index
        for name, size in reversed(list(zip(names, sizes))):
            at[name] = rest % size
            rest //= size
        away = 0.0
        if "row_0" in at:
            away += hops(at["row_0"], full["row_0"] // 2, full["row_0"])
        if "col_0" in at:
            away += hops(at["col_0"], middle, full["col_0"])
        if "row_1" in at:
            away += hops(at["row_1"] * full["col_1"] + at["col_1"], y_size // 2, y_size)
        elif "col_1" in at:
            away += at["col_1"]
        if "col_2" in at:
            away += 0.5 * (full["col_2"] - 1 - at["col_2"])
        places.append((-away, index))
    root = max(places)
    return [root[1]] + [p[1] for p in sorted(places) if p != root]


def exchange(payload, axis, order):
    return lax.all_to_all(payload, axis, 0, 0, axis_index_groups=[order], tiled=True)


def per_device(boxes, pins, capacity, cell_bin, cell_area):
    tile_rows, tile_cols = capacity.shape
    rows, cols = lax.axis_size(ROW), lax.axis_size(COL)
    groups = lax.axis_size("col_0")
    nets = boxes.shape[1]
    cells = cell_bin.shape[1]
    factor = 2.0 / (tile_rows * rows)
    near = lax.axis_size(NEAR)
    col_order = peer_order(COL)
    near_order = peer_order(NEAR)
    far_order = peer_order(("col_0",))
    pins = pins.reshape(1, nets)
    below, cell_sums = call(
        functools.partial(cells_kernel, tile_rows, tile_cols),
        [(tile_rows, tile_cols), (8, LANES)],
        (cell_bin, cell_area),
        flops=4_000_000_000,
    )

    def one_round(base, past):
        (packed,) = call(
            functools.partial(
                pack_kernel, col_order, cols, groups, tile_cols * (cols // groups), tile_rows
            ),
            [(cols, 8, SLOTS)],
            (boxes, pins) + base,
            [pltpu.VMEM((16, nets), F32)],
        )
        mine = exchange(packed, COL, col_order)
        rudy, pay = call(
            functools.partial(tile_kernel, past is not None),
            [(tile_rows, tile_cols), (near * 4, LANES)],
            (mine, capacity, below, cell_sums)
            + (() if past is None else (past,)),
            limit=28,
        )
        pays = exchange(pay.reshape(near, 4, LANES), NEAR, near_order).reshape(near * 4, LANES)
        one = jax.ShapeDtypeStruct((1,), jnp.int32)
        carried, totals, reached, left = call(
            functools.partial(carry_kernel, near_order, rows),
            [(8, LANES), (groups, LANES), one, one],
            (pays,) + base,
        )
        return left, reached, rudy, carried, totals

    def unfinished(state):
        return state[0][0] > 0

    def next_round(state):
        return one_round((state[1],), state[2])

    first = one_round((), None)
    _, _, rudy, carried, totals = lax.cond(
        unfinished(first),
        lambda state: lax.while_loop(unfinished, next_round, state),
        lambda state: state,
        first,
    )

    totals = exchange(totals, "col_0", far_order)
    shape = (cells // LANES, LANES)
    inflation, looked = call(
        functools.partial(inflation_kernel, factor),
        [(tile_rows, tile_cols), (1, cells)],
        (rudy, capacity, cell_bin, carried),
        limit=28,
        flops=4_000_000_000,
    )
    (sizes,) = call(
        functools.partial(sizes_kernel, factor),
        [shape],
        (carried, totals, cell_bin.reshape(shape), cell_area.reshape(shape), looked.reshape(shape)),
    )
    return rudy, inflation, sizes.reshape(cell_area.shape)


def solution(mesh):
    split = Mesh(mesh.devices.reshape(4, 2, 8, 2, 2), ROW + COL)
    placed = (P(None, COL), P(COL), P(ROW, COL), P(ROW, COL), P(ROW, COL))
    return jax.shard_map(
        per_device,
        mesh=split,
        in_specs=placed,
        out_specs=(P(ROW, COL), P(ROW, COL), P(ROW, COL)),
        check_vma=False,
    )
```
